256 devices in a mesh: wa: 64 (over x_hi, y, z), ba: 4 (over x_lo, core).
Axes of the slice: x: 4 (x_hi: 2, x_lo: 2; x = x_hi * 2 + x_lo), y: 4, z: 8, core: 2. Of those that a mesh axis runs over, the one named last changes fastest.
Arguments:
- latent: float32 [16, 8, 8192], P('ba', None, 'wa'), parts along dimension 0, may hold values from -12 to 12
- noise: float32 [2, 16, 8, 8192], P(None, 'ba', None, 'wa'), parts along dimension 1, may hold values from -6 to 6
- offsets: int32 [128], P('wa'), may hold values from 0 to 63
- anchors: int32 [2], replicated, may hold values from 0 to 127
- guidance: float32 [1], replicated, may hold values from 0.4 to 0.8
- w_in: bfloat16 [320, 36], replicated, may hold values from -1 to 1
- w_mid: bfloat16 [320, 320], replicated, may hold values from -0.3125 to 0.3125
- w_out: bfloat16 [36, 320], replicated, may hold values from -0.109375 to 0.109375
- t_embed: float32 [2, 320], replicated, may hold values from -6 to 6
- w_feat: float32 [64, 4], replicated, may hold values from -3 to 3
Outputs:
- denoised: float32 [16, 8, 8192], P('ba', None, 'wa'), parts along dimension 0
The draws below stay inside these ranges and needn't reach their ends.
There are 4 independent parts, one for each index of `ba`. The reference program is written for one: setup_inputs(seed, part) draws one part's arguments, and reference() takes and returns one part's arrays. A program takes and returns all parts, laid end to end along the dimension named above; an argument that names none is the same for every part. Nothing has to cross between parts.
All inputs are finite; a program needn't handle non-finite values.
Results may differ from the reference program's by a relative error of at most 0.0065.
Values sent between devices are 32-bit elements; how exact they have to be, the bound alone decides.
No kernel may reach another device: no remote copies, remote signals or barrier semaphores. Data moves between devices by JAX's collectives and lax.ppermute only.
A program may use at most 64 MiB of HBM per device.

```python
import math
import jax
import jax.numpy as jnp
from jax import lax

C = 4
HID = 320
FEAT = 64
H = 8
WIN = 128
STRIDE = 64
STEPS = 2
NWIN = 128
W = 8192


def draw_latent(key, part):
    base_key = jax.random.fold_in(key, 7)
    normal_key = jax.random.fold_in(base_key, 0)
    columns = jnp.arange(W, dtype=jnp.float32)
    rising = 2.0 ** (columns / W)
    values = jax.random.normal(normal_key, (C, H, W), jnp.float32)
    return jnp.clip(values * rising, -12.0, 12.0)


def place_ends(values, own_key, smallest, largest):
    spot = [jax.random.randint(jax.random.fold_in(own_key, axis), (), 0, length) for axis, length in enumerate(values.shape)]
    longest = values.shape.index(max(values.shape))
    neighbour = spot[:longest] + [(spot[longest] + 1) % values.shape[longest]] + spot[longest + 1:]
    return values.at[tuple(spot)].set(smallest).at[tuple(neighbour)].set(largest)


def levels(stream_key, extent, cuts, low, top_value):
    def one(dim, parts):
        steps = jax.random.uniform(jax.random.fold_in(jax.random.fold_in(stream_key, 6), dim), (parts,), jnp.float32, low / len(cuts), top_value / len(cuts))
        return jnp.repeat(jnp.exp(steps), extent[dim] // parts).reshape((-1,) + (1,) * (len(extent) - dim - 1))

    loudness = one(*cuts[0])
    for cut in cuts[1:]:
        loudness = loudness * one(*cut)
    return loudness


def normal_values(stream_key, extent, scale, bound, shards=(), kind=jnp.bfloat16):
    values = jax.random.normal(stream_key, extent, jnp.float32) * scale
    if len(shards) > 0:
        values = levels(stream_key, extent, shards, -0.22, 0.18) * values
    return jnp.clip(values, min=-bound, max=bound).astype(kind)


def setup_inputs(seed: int = 0, part: int = 0) -> dict:
    key_list = jax.random.split(jax.random.key(seed), 11)
    own_keys = jax.random.split(jax.random.fold_in(key_list[10], part), 11)
    latent = draw_latent(jax.random.fold_in(jax.random.fold_in(key_list[10], part), 71), part)
    noise = normal_values(own_keys[1], (STEPS, C, H, W), 1.0, 6.0, ((3, 64),), jnp.float32)
    offsets = place_ends(jax.random.randint(key_list[2], (NWIN,), 0, STRIDE), jax.random.fold_in(key_list[2], 1), 0, STRIDE - 1).astype(jnp.int32)
    anchors = jax.random.randint(key_list[3], (STEPS,), 0, NWIN).astype(jnp.int32)
    guidance = jnp.clip(jax.random.uniform(key_list[4], (1,), jnp.float32, 0.4, 0.8), 0.4, 0.8)
    w_in = normal_values(key_list[5], (HID, 9 * C), (9 * C) ** -0.5, 1.0)
    w_mid = normal_values(key_list[6], (HID, HID), HID ** -0.5, 0.3125)
    w_out = normal_values(key_list[7], (9 * C, HID), (9 * HID) ** -0.5, 0.109375)
    t_embed = normal_values(key_list[8], (STEPS, HID), 1.0, 6.0, (), jnp.float32)
    w_feat = normal_values(key_list[9], (FEAT, C), C ** -0.5, 3.0, (), jnp.float32)
    return {"latent": latent, "noise": noise, "offsets": offsets, "anchors": anchors, "guidance": guidance, "w_in": w_in, "w_mid": w_mid, "w_out": w_out, "t_embed": t_embed, "w_feat": w_feat}


TAP_SHIFTS = ((-1, -1), (-1, 0), (-1, 1), (0, -1), (0, 0), (0, 1), (1, -1), (1, 0), (1, 1))
CUMULATIVE_ALPHA = (0.35, 0.55, 0.72, 0.85, 0.93)
STABILITY = 1e-06

def plan(number):
    current = CUMULATIVE_ALPHA[number]
    following = CUMULATIVE_ALPHA[number + 1]
    spread = 0.3 * math.sqrt(1.0 - following)
    return (math.sqrt(current), math.sqrt(1.0 - current), math.sqrt(following), math.sqrt(1.0 - following - spread * spread), spread)

def tapped(field):
    height, columns = (field.shape[-2], field.shape[-1])
    padding = [(0, 0)] * (field.ndim - 2) + [(1, 1), (1, 1)]
    padded = jnp.pad(field, padding)
    return jnp.stack([padded[..., 1 + down_by:1 + down_by + height, 1 + right_by:1 + right_by + columns] for down_by, right_by in TAP_SHIFTS])

def denoise(window, w_in, w_mid, w_out, embedding):
    channels, height, columns = window.shape
    stacked = tapped(window.astype(jnp.bfloat16)).reshape(9 * channels, height * columns)
    hidden_in = jnp.dot(w_in, stacked, preferred_element_type=jnp.float32) + embedding[:, None]
    activated = jax.nn.silu(hidden_in).astype(jnp.bfloat16)
    middle = jnp.dot(w_mid, activated, preferred_element_type=jnp.float32)
    joined = (hidden_in + jax.nn.silu(middle)).astype(jnp.bfloat16)
    outward = jnp.dot(w_out, joined, preferred_element_type=jnp.float32).reshape(9, channels, height, columns)
    padded = jnp.pad(outward, ((0, 0), (0, 0), (1, 1), (1, 1)))
    result = jnp.zeros((channels, height, columns), jnp.float32)
    for index, (down_by, right_by) in enumerate(TAP_SHIFTS):
        result = result + padded[index, :, 1 + down_by:1 + down_by + height, 1 + right_by:1 + right_by + columns]
    return result

def clean_of(windows, w_in, w_mid, w_out, embedding, now_a, now_s):
    predicted = jax.vmap(denoise, (0, None, None, None, None))(windows, w_in, w_mid, w_out, embedding)
    cleaned = (windows - now_s * predicted) / now_a
    return (cleaned, predicted)

def percept(cleaned, w_feat):
    return jax.nn.silu(jnp.einsum('fc,chw->fhw', w_feat, cleaned, precision=lax.Precision.HIGHEST))

def mismatch(cleaned, anchor_percept, w_feat):
    difference = percept(cleaned, w_feat) - anchor_percept
    return 0.5 * jnp.sum(difference * difference) / w_feat.shape[0]

def finish_gradient(cleaned, pullback, anchor_percept, w_feat):
    clean_grad = jax.vmap(jax.grad(mismatch), (0, None, None))(cleaned, anchor_percept, w_feat)
    return pullback(clean_grad)[0]

def advance(windows, gradient, predicted, scale, now_a, now_s, next_a, direction):
    return next_a * (windows - scale * gradient - now_s * predicted) / now_a + direction * predicted

def reference(latent, noise, offsets, anchors, guidance, w_in, w_mid, w_out, t_embed, w_feat):
    channels, height, width = latent.shape
    window_count = offsets.shape[0]
    per_block = WIN // STRIDE
    starts = jnp.arange(window_count, dtype=jnp.int32) * STRIDE + offsets
    positions = jnp.arange(width + WIN, dtype=jnp.int32)
    inside = (positions[None, :] >= starts[:, None]) & (positions[None, :] < starts[:, None] + WIN)
    cover = lax.optimization_barrier(jnp.sum(inside.astype(jnp.float32), axis=0))
    counts = cover[:width].at[:WIN].add(cover[width:])
    block_starts = starts.reshape(window_count // per_block, per_block)
    state = latent
    for number in range(STEPS):
        now_a, now_s, next_a, direction, spread = plan(number)
        embedding = t_embed[number]
        padded_state = jnp.concatenate([state, state[:, :, :WIN]], axis=2)

        def cut_window(root):
            return lax.dynamic_slice_in_dim(padded_state, root, WIN, 2)

        def forward(roots):
            windows = jax.vmap(cut_window)(roots)
            return clean_of(windows, w_in, w_mid, w_out, embedding, now_a, now_s)[0]
        cleaned_all = lax.map(forward, block_starts).reshape(window_count, channels, height, WIN)
        anchor_clean = lax.dynamic_index_in_dim(cleaned_all, anchors[number], 0, keepdims=False)
        anchor_percept = percept(anchor_clean, w_feat)

        def backward(roots):
            windows = jax.vmap(cut_window)(roots)

            def cleaning(inputs):
                return clean_of(inputs, w_in, w_mid, w_out, embedding, now_a, now_s)
            cleaned, pullback, predicted = jax.vjp(cleaning, windows, has_aux=True)
            gradient = finish_gradient(cleaned, pullback, anchor_percept, w_feat)
            return (gradient, predicted, jnp.sum(gradient * gradient))
        gradients, predictions, squares = lax.map(backward, block_starts)
        mean_square = jnp.sum(squares) / (window_count * channels * height * WIN)
        scale = guidance[0] * lax.rsqrt(mean_square + STABILITY)
        windows = jax.vmap(cut_window)(starts)
        advanced = advance(windows, gradients.reshape(windows.shape), predictions.reshape(windows.shape), scale, now_a, now_s, next_a, direction)

        def place(summed, element):
            root, piece = element
            current = lax.dynamic_slice_in_dim(summed, root, WIN, 2)
            return (lax.dynamic_update_slice_in_dim(summed, current + piece, root, 2), None)
        summed = lax.scan(place, jnp.zeros((channels, height, width + WIN), jnp.float32), (starts, advanced))[0]
        blended = summed[:, :, :width].at[:, :, :WIN].add(summed[:, :, width:])
        state = blended / counts + spread * noise[number]
    return state
```

```python
import functools
import math

import jax
import jax.numpy as jnp
from jax import lax
from jax.experimental import pallas as pl
from jax.experimental.pallas import tpu as pltpu
from jax.sharding import Mesh
from jax.sharding import PartitionSpec as P

C = 4
H = 8
HID = 320
FEAT = 64
WIN = 128
STRIDE = 64
NDEV = 64
NWIN = 128
TAPS = 9 * C
FIELD = H * WIN
CHUNK = 512
WA = ("wa_0", "wa_1", "wa_2")
NEAR = "wa_2"
FAR = ("wa_0", "wa_1")
GROUP = 8

TAP_SHIFTS = ((-1, -1), (-1, 0), (-1, 1), (0, -1), (0, 0), (0, 1), (1, -1), (1, 0), (1, 1))
CUMULATIVE_ALPHA = (0.35, 0.55, 0.72, 0.85, 0.93)
STABILITY = 1e-06
ELEMENTS = float(NWIN * C * H * WIN)
F32 = jnp.float32
BF16 = jnp.bfloat16


def plan(number):
    current = CUMULATIVE_ALPHA[number]
    following = CUMULATIVE_ALPHA[number + 1]
    spread = 0.3 * math.sqrt(1.0 - following)
    return (
        math.sqrt(current),
        math.sqrt(1.0 - current),
        math.sqrt(following),
        math.sqrt(1.0 - following - spread * spread),
        spread,
    )


def lanes(shape=(C, H, WIN)):
    return lax.broadcasted_iota(jnp.int32, shape, len(shape) - 1)


def shift_rows(x, by):
    if by == 0:
        return x
    row = lax.broadcasted_iota(jnp.int32, x.shape, 1)
    inside = row >= 1 if by < 0 else row < H - 1
    return jnp.where(inside, pltpu.roll(x, (-by) % H, 1), 0.0)


def shift_lanes(x, by):
    if by == 0:
        return x
    lane = lanes(x.shape)
    inside = lane >= 1 if by < 0 else lane < WIN - 1
    return jnp.where(inside, pltpu.roll(x, (-by) % WIN, 2), 0.0)


def spread_taps(x, sign, tall):
    moved = {by: shift_lanes(x, sign * by) for by in (-1, 0, 1)}
    for k, (down, right) in enumerate(TAP_SHIFTS):
        tall[32 * k : 32 * (k + 1), :] = shift_rows(moved[right], sign * down).reshape(32, WIN)
    rows = [tall[pl.ds(h, TAPS, stride=H), :] for h in range(H)]
    return jnp.concatenate(rows, axis=1).astype(BF16)


def store_taps(tall, first, values):
    for j in range(values.shape[1] // WIN):
        tall[pl.ds(first + j, TAPS, stride=H), :] = values[:, WIN * j : WIN * (j + 1)]


def gather_taps(tall, sign):
    total = None
    for right in (-1, 0, 1):
        part = None
        for k, (down, across) in enumerate(TAP_SHIFTS):
            if across == right:
                piece = tall[32 * k : 32 * (k + 1), :].reshape(C, H, WIN)
                piece = shift_rows(piece, sign * down)
                part = piece if part is None else part + piece
        part = shift_lanes(part, sign * right)
        total = part if total is None else total + part
    return total


def silu_and_slope(v):
    u = 0.5 * v
    t = jnp.tanh(u)
    s = u + u * t
    g = 0.5 + 0.5 * t
    return s, g + s * (1.0 - g)


def silu(v):
    u = 0.5 * v
    return u + u * jnp.tanh(u)


def dot(a, b):
    return lax.dot_general(a, b, (((1,), (0,)), ((), ())), preferred_element_type=F32)


def predict(window, weights, embed, tall, slopes, slot):
    taps = spread_taps(window, 1, tall)
    for start in range(0, FIELD, CHUNK):
        hidden = dot(weights["w_in"][...], taps[:, start : start + CHUNK]) + embed
        if slopes is None:
            active = silu(hidden)
            joined = hidden + silu(dot(weights["w_mid"][...], active.astype(BF16)))
        else:
            at = pl.ds(slot * FIELD + start, CHUNK)
            active, slopes[0][:, at] = silu_and_slope(hidden)
            more, slopes[1][:, at] = silu_and_slope(dot(weights["w_mid"][...], active.astype(BF16)))
            joined = hidden + more
        store_taps(tall, start // WIN, dot(weights["w_out"][...], joined.astype(BF16)))
    return gather_taps(tall, 1)


def pull_back(cotangent, weights, tall, slopes, slot):
    taps = spread_taps(cotangent, -1, tall)
    for start in range(0, FIELD, CHUNK):
        at = pl.ds(slot * FIELD + start, CHUNK)
        d_joined = dot(weights["w_out_t"][...], taps[:, start : start + CHUNK])
        d_middle = (d_joined * slopes[1][:, at]).astype(BF16)
        d_hidden = d_joined + dot(weights["w_mid_t"][...], d_middle) * slopes[0][:, at]
        store_taps(tall, start // WIN, dot(weights["w_in_t"][...], d_hidden.astype(BF16)))
    return gather_taps(tall, -1)


def percept_pull_back(cleans, anchor, w_feat):
    grads = [[jnp.zeros((H, WIN), F32) for _ in range(C)] for _ in cleans]
    for f in range(FEAT):
        w = [w_feat[f * C + c] for c in range(C)]

        def mixed(x):
            return (w[0] * x[0] + w[1] * x[1]) + (w[2] * x[2] + w[3] * x[3])

        target = silu(mixed(anchor))
        for x, grad in zip(cleans, grads):
            s, slope = silu_and_slope(mixed(x))
            d = (s - target) * slope
            for c in range(C):
                grad[c] = grad[c] + w[c] * d
    return [jnp.stack(grad) * (1.0 / FEAT) for grad in grads]


def cut(first, second, start):
    by = (WIN - start) % WIN
    return jnp.where(
        lanes() < WIN - start, pltpu.roll(first, by, 2), pltpu.roll(second, by, 2)
    )


def place(pieces, starts):
    own, spill = 0.0, 0.0
    for piece, start in zip(pieces, starts):
        moved = pltpu.roll(piece, start, 2)
        inside = lanes() >= start
        own = own + jnp.where(inside, moved, 0.0)
        spill = spill + jnp.where(inside, 0.0, moved)
    return own, spill


def step(number, first, second, starts, anchor, weights, embed_ref, w_feat, scratch):
    now_a, now_s, next_a, direction, _ = plan(number)
    talls, slopes = scratch[:3], scratch[3:]
    embed = jnp.broadcast_to(embed_ref[:, number : number + 1], (HID, CHUNK))
    windows = [cut(first, second, start) for start in starts]
    predicted = [
        predict(windows[i], weights, embed, talls[i], slopes, i) for i in range(2)
    ]
    anchor_predicted = predict(anchor, weights, embed, talls[2], None, 2)
    cleans = [(w - now_s * p) * (1.0 / now_a) for w, p in zip(windows, predicted)]
    anchor_clean = (anchor - now_s * anchor_predicted) * (1.0 / now_a)
    d_cleans = percept_pull_back(cleans, anchor_clean, w_feat)
    gradients = [
        d * (1.0 / now_a)
        + pull_back(d * (-now_s / now_a), weights, talls[i], slopes, i)
        for i, d in enumerate(d_cleans)
    ]
    square = sum(jnp.sum(g * g, axis=0) for g in gradients)
    plain = [
        (next_a / now_a) * (w - now_s * p) + direction * p for w, p in zip(windows, predicted)
    ]
    plain_own, plain_spill = place(plain, starts)
    steep_own, steep_spill = place([g * (-next_a / now_a) for g in gradients], starts)
    return plain_own, plain_spill, steep_own, steep_spill, square


def scale_of(total, guidance):
    return guidance[0] * lax.rsqrt(jnp.full((1, 1, 1), total) * (1.0 / ELEMENTS) + STABILITY)


def opening_kernel(me_ref, anchors, offsets, latent, noise, share, halo):
    me = me_ref[0]
    owner = anchors[0] // 2
    own = latent[...]
    x = jnp.where(me == owner, own, 0.0)
    y = jnp.where(me == (owner + 1) % NDEV, own, 0.0)
    lane = lanes((H, WIN))
    known = jnp.where(
        lane == 2 * me,
        offsets[0].astype(F32),
        jnp.where(lane == 2 * me + 1, offsets[1].astype(F32), 0.0),
    )
    for i in range(GROUP):
        share[i, 0:4] = x
        share[i, 4:8] = y
        share[i, 8] = known
    halo[0:4] = own
    halo[4:8] = noise[0]


def relay_kernel(got, share):
    total = got[0]
    for i in range(1, GROUP):
        total = total + got[i]
    for i in range(GROUP):
        share[i] = total


def weights_of(refs):
    names = ("w_in", "w_mid", "w_out", "w_in_t", "w_mid_t", "w_out_t")
    return dict(zip(names, refs))


def first_kernel(
    me_ref, anchors, offsets, w_feat, latent, noise, halo, shared,
    w_in, w_mid, w_out, w_in_t, w_mid_t, w_out_t, embed,
    share, own_out, spill_out, inverse, *scratch,
):
    weights = weights_of((w_in, w_mid, w_out, w_in_t, w_mid_t, w_out_t))
    me = me_ref[0]
    total = shared[0]
    for i in range(1, GROUP):
        total = total + shared[i]
    table = total[8]
    lane = lanes((H, WIN))

    def offset_of(window):
        picked = jnp.where(lane == window, table, 0.0)[0:1]
        return jnp.sum(picked).astype(jnp.int32)

    starts = (offsets[0], STRIDE + offsets[1])
    anchor_at = (anchors[0] % 2) * STRIDE + offset_of(anchors[0])
    anchor = cut(total[0:4], total[4:8], anchor_at)
    plain_own, plain_spill, steep_own, steep_spill, square = step(
        0, latent[...], halo[0:4], starts, anchor, weights, embed, w_feat, scratch
    )
    spread = plan(0)[-1]

    def covered(windows):
        count = jnp.zeros((H, WIN), F32)
        for begin in windows:
            count = count + jnp.where((lane >= begin) & (lane < begin + WIN), 1.0, 0.0)
        return 1.0 / count

    left, right = 2 * me + NWIN - 2, 2 * me + 2
    before = (
        offset_of(left % NWIN) - WIN,
        offset_of((left + 1) % NWIN) - STRIDE,
    )
    after = (offset_of(right % NWIN), STRIDE + offset_of((right + 1) % NWIN))
    inverse_own = covered(before + starts)
    inverse_next = covered((starts[0] - WIN, starts[1] - WIN) + after)
    inverse[0] = inverse_own
    inverse[1] = inverse_next
    own_out[0:4] = plain_own
    own_out[4:8] = steep_own
    spill_out[0:4] = plain_spill
    spill_out[4:8] = steep_spill

    owner = anchors[1] // 2
    next_at = (anchors[1] % 2) * STRIDE + offset_of(anchors[1])
    here, ahead, behind = (
        me == owner, me == (owner + 1) % NDEV, me == (owner + NDEV - 1) % NDEV
    )

    def portion(own, spill):
        x = jnp.where(here, own, jnp.where(behind, spill, 0.0))
        y = jnp.where(here, spill, jnp.where(ahead, own, 0.0))
        return cut(x, y, next_at)

    plain_part = portion(
        plain_own * inverse_own + spread * noise[0], plain_spill * inverse_next
    )
    steep_part = portion(steep_own * inverse_own, steep_spill * inverse_next)
    for i in range(GROUP):
        share[i, 0:4] = plain_part
        share[i, 4:8] = steep_part
        share[i, 8] = square


def second_kernel(
    offsets, w_feat, guidance, noise, halo, shared, own_in, spill_in, spill_left, own_right, inverse,
    w_in, w_mid, w_out, w_in_t, w_mid_t, w_out_t, embed,
    own_out, spill_out, square_out, *scratch,
):
    weights = weights_of((w_in, w_mid, w_out, w_in_t, w_mid_t, w_out_t))
    total = shared[0]
    for i in range(1, GROUP):
        total = total + shared[i]
    scale = scale_of(jnp.sum(total[8]), guidance)
    spread = plan(0)[-1]
    anchor = total[0:4] + scale * total[4:8]
    own = own_in[...] + spill_left[...]
    beyond = spill_in[...] + own_right[...]
    first = (own[0:4] + scale * own[4:8]) * inverse[0] + spread * noise[0]
    second = (beyond[0:4] + scale * beyond[4:8]) * inverse[1] + spread * halo[4:8]
    starts = (offsets[0], STRIDE + offsets[1])
    plain_own, plain_spill, steep_own, steep_spill, square = step(
        1, first, second, starts, anchor, weights, embed, w_feat, scratch
    )
    own_out[0:4] = plain_own
    own_out[4:8] = steep_own
    spill_out[0:4] = plain_spill
    spill_out[4:8] = steep_spill
    row = jnp.sum(square, axis=0, keepdims=True)
    square_out[...] = jnp.broadcast_to(row[None], (NDEV, 1, WIN))


def closing_kernel(guidance, squares, own_in, spill_left, inverse, noise, out):
    scale = scale_of(jnp.sum(squares[...]), guidance)
    own = own_in[...] + spill_left[...]
    spread = plan(1)[-1]
    out[...] = (own[0:4] + scale * own[4:8]) * inverse[0] + spread * noise[1]


def call(kernel, shapes, n_scalars, *args, scratch=()):
    in_specs = [
        pl.BlockSpec(memory_space=pltpu.SMEM if i < n_scalars else pltpu.VMEM)
        for i in range(len(args))
    ]
    return pl.pallas_call(
        kernel,
        out_shape=[jax.ShapeDtypeStruct(shape, F32) for shape in shapes],
        in_specs=in_specs,
        out_specs=[pl.BlockSpec(memory_space=pltpu.VMEM) for _ in shapes],
        scratch_shapes=scratch,
        name=kernel.__name__,
    )(*args)


def scratches():
    return [pltpu.VMEM((8 * TAPS, WIN), F32)] * 3 + [pltpu.VMEM((HID, 2 * FIELD), F32)] * 2


def exchanged(shares, axes):
    return lax.all_to_all(shares, axes, split_axis=0, concat_axis=0, tiled=True)


def passed_along(shard, by):
    return lax.ppermute(shard, WA, [(i, (i + by) % NDEV) for i in range(NDEV)])


def local(latent, noise, offsets, anchors, guidance, w_in, w_mid, w_out, t_embed, w_feat):
    me = lax.axis_index(WA).astype(jnp.int32).reshape(1)
    features = w_feat.reshape(-1)
    weights = (w_in, w_mid, w_out, w_in.T, w_mid.T, w_out.T, t_embed.T)
    blocks, group = (8, H, WIN), (GROUP, 9, H, WIN)

    share, halo = call(opening_kernel, (group, blocks), 3, me, anchors, offsets, latent, noise)
    halo = passed_along(halo, -1)
    (share,) = call(relay_kernel, (group,), 0, exchanged(share, NEAR))
    share = exchanged(share, FAR)

    share, own, spill, inverse = call(
        first_kernel, (group, blocks, blocks, (2, H, WIN)), 4,
        me, anchors, offsets, features, latent, noise, halo, share, *weights,
        scratch=scratches(),
    )
    spill_left = passed_along(spill, 1)
    own_right = passed_along(own, -1)
    (share,) = call(relay_kernel, (group,), 0, exchanged(share, NEAR))
    share = exchanged(share, FAR)

    own, spill, squares = call(
        second_kernel, (blocks, blocks, (NDEV, 1, WIN)), 3,
        offsets, features, guidance, noise, halo, share, own, spill, spill_left, own_right,
        inverse, *weights,
        scratch=scratches(),
    )
    spill_left = passed_along(spill, 1)
    squares = exchanged(squares, WA)
    (out,) = call(
        closing_kernel, ((C, H, WIN),), 1, guidance, squares, own, spill_left, inverse, noise
    )
    return out


def solution(mesh):
    finer = Mesh(mesh.devices.reshape(2, 4, 8, mesh.shape["ba"]), ("wa_0", "wa_1", "wa_2", "ba"))
    placed = (P("ba", None, WA), P(None, "ba", None, WA), P(WA), P(), P(), P(), P(), P(), P(), P())
    return jax.shard_map(
        local, mesh=finer, in_specs=placed, out_specs=P("ba", None, WA), check_vma=False
    )
```

```python
import math

import jax
import jax.numpy as jnp
from jax import lax
from jax.experimental import pallas as pl
from jax.experimental.pallas import tpu as pltpu
from jax.sharding import Mesh
from jax.sharding import PartitionSpec as P

C = 4
H = 8
HID = 320
FEAT = 64
WIN = 128
STRIDE = 64
NDEV = 64
NWIN = 128
TAPS = 9 * C
FIELD = H * WIN
CHUNK = 512
WA = ("wa_0", "wa_1", "wa_2")
NEAR = "wa_2"
FAR = ("wa_0", "wa_1")
GROUP = 8

TAP_SHIFTS = ((-1, -1), (-1, 0), (-1, 1), (0, -1), (0, 0), (0, 1), (1, -1), (1, 0), (1, 1))
CUMULATIVE_ALPHA = (0.35, 0.55, 0.72, 0.85, 0.93)
STABILITY = 1e-06
ELEMENTS = float(NWIN * C * H * WIN)
F32 = jnp.float32
BF16 = jnp.bfloat16


def plan(number):
    current = CUMULATIVE_ALPHA[number]
    following = CUMULATIVE_ALPHA[number + 1]
    spread = 0.3 * math.sqrt(1.0 - following)
    return (
        math.sqrt(current),
        math.sqrt(1.0 - current),
        math.sqrt(following),
        math.sqrt(1.0 - following - spread * spread),
        spread,
    )


def lanes(shape=(C, H, WIN)):
    return lax.broadcasted_iota(jnp.int32, shape, len(shape) - 1)


def shift_rows(x, by):
    if by == 0:
        return x
    row = lax.broadcasted_iota(jnp.int32, x.shape, 1)
    inside = row >= 1 if by < 0 else row < H - 1
    return jnp.where(inside, pltpu.roll(x, (-by) % H, 1), 0.0)


def shift_lanes(x, by):
    if by == 0:
        return x
    lane = lanes(x.shape)
    inside = lane >= 1 if by < 0 else lane < WIN - 1
    return jnp.where(inside, pltpu.roll(x, (-by) % WIN, 2), 0.0)


def spread_taps(x, sign, tall):
    moved = {by: shift_lanes(x, sign * by) for by in (-1, 0, 1)}
    for k, (down, right) in enumerate(TAP_SHIFTS):
        tall[32 * k : 32 * (k + 1), :] = shift_rows(moved[right], sign * down).reshape(32, WIN)
    rows = [tall[pl.ds(h, TAPS, stride=H), :] for h in range(H)]
    return jnp.concatenate(rows, axis=1).astype(BF16)


def store_taps(tall, first, values):
    for j in range(values.shape[1] // WIN):
        tall[pl.ds(first + j, TAPS, stride=H), :] = values[:, WIN * j : WIN * (j + 1)]


def gather_taps(tall, sign):
    total = None
    for right in (-1, 0, 1):
        part = None
        for k, (down, across) in enumerate(TAP_SHIFTS):
            if across == right:
                piece = tall[32 * k : 32 * (k + 1), :].reshape(C, H, WIN)
                piece = shift_rows(piece, sign * down)
                part = piece if part is None else part + piece
        part = shift_lanes(part, sign * right)
        total = part if total is None else total + part
    return total


def silu_and_slope(v):
    u = 0.5 * v
    t = jnp.tanh(u)
    s = u + u * t
    g = 0.5 + 0.5 * t
    return s, g + s * (1.0 - g)


def silu(v):
    u = 0.5 * v
    return u + u * jnp.tanh(u)


def dot(a, b):
    return lax.dot_general(a, b, (((1,), (0,)), ((), ())), preferred_element_type=F32)


def predict(window, weights, embed, tall, slopes, slot):
    taps = spread_taps(window, 1, tall)
    for start in range(0, FIELD, CHUNK):
        hidden = dot(weights["w_in"][...], taps[:, start : start + CHUNK]) + embed
        if slopes is None:
            active = silu(hidden)
            joined = hidden + silu(dot(weights["w_mid"][...], active.astype(BF16)))
        else:
            at = pl.ds(slot * FIELD + start, CHUNK)
            active, slopes[0][:, at] = silu_and_slope(hidden)
            more, slopes[1][:, at] = silu_and_slope(dot(weights["w_mid"][...], active.astype(BF16)))
            joined = hidden + more
        store_taps(tall, start // WIN, dot(weights["w_out"][...], joined.astype(BF16)))
    return gather_taps(tall, 1)


def pull_back(cotangent, weights, tall, slopes, slot):
    taps = spread_taps(cotangent, -1, tall)
    for start in range(0, FIELD, CHUNK):
        at = pl.ds(slot * FIELD + start, CHUNK)
        d_joined = dot(weights["w_out_t"][...], taps[:, start : start + CHUNK])
        d_middle = (d_joined * slopes[1][:, at]).astype(BF16)
        d_hidden = d_joined + dot(weights["w_mid_t"][...], d_middle) * slopes[0][:, at]
        store_taps(tall, start // WIN, dot(weights["w_in_t"][...], d_hidden.astype(BF16)))
    return gather_taps(tall, -1)


def percept_pull_back(cleans, anchor, w_feat):
    grads = [[jnp.zeros((H, WIN), F32) for _ in range(C)] for _ in cleans]
    for f in range(FEAT):
        w = [w_feat[f * C + c] for c in range(C)]

        def mixed(x):
            return (w[0] * x[0] + w[1] * x[1]) + (w[2] * x[2] + w[3] * x[3])

        target = silu(mixed(anchor))
        for x, grad in zip(cleans, grads):
            s, slope = silu_and_slope(mixed(x))
            d = (s - target) * slope
            for c in range(C):
                grad[c] = grad[c] + w[c] * d
    return [jnp.stack(grad) * (1.0 / FEAT) for grad in grads]


def cut(first, second, start):
    by = (WIN - start) % WIN
    return jnp.where(
        lanes() < WIN - start, pltpu.roll(first, by, 2), pltpu.roll(second, by, 2)
    )


def place(pieces, starts):
    own, spill = 0.0, 0.0
    for piece, start in zip(pieces, starts):
        moved = pltpu.roll(piece, start, 2)
        inside = lanes() >= start
        own = own + jnp.where(inside, moved, 0.0)
        spill = spill + jnp.where(inside, 0.0, moved)
    return own, spill


def step(number, first, second, starts, anchor, weights, embed_ref, w_feat, scratch):
    now_a, now_s, next_a, direction, _ = plan(number)
    talls, slopes = scratch[:3], scratch[3:]
    embed = jnp.broadcast_to(embed_ref[:, number : number + 1], (HID, CHUNK))
    windows = [cut(first, second, start) for start in starts]
    predicted = [
        predict(windows[i], weights, embed, talls[i], slopes, i) for i in range(2)
    ]
    anchor_predicted = predict(anchor, weights, embed, talls[2], None, 2)
    cleans = [(w - now_s * p) * (1.0 / now_a) for w, p in zip(windows, predicted)]
    anchor_clean = (anchor - now_s * anchor_predicted) * (1.0 / now_a)
    d_cleans = percept_pull_back(cleans, anchor_clean, w_feat)
    gradients = [
        d * (1.0 / now_a)
        + pull_back(d * (-now_s / now_a), weights, talls[i], slopes, i)
        for i, d in enumerate(d_cleans)
    ]
    square = sum(jnp.sum(g * g, axis=0) for g in gradients)
    plain = [
        (next_a / now_a) * (w - now_s * p) + direction * p for w, p in zip(windows, predicted)
    ]
    plain_own, plain_spill = place(plain, starts)
    steep_own, steep_spill = place([g * (-next_a / now_a) for g in gradients], starts)
    return plain_own, plain_spill, steep_own, steep_spill, square


def scale_of(total, guidance):
    return guidance[0] * lax.rsqrt(jnp.full((1, 1, 1), total) * (1.0 / ELEMENTS) + STABILITY)


def opening_kernel(me_ref, anchors, offsets, latent, noise, share, halo):
    me = me_ref[0]
    owner = anchors[0] // 2
    own = latent[...]
    x = jnp.where(me == owner, own, 0.0)
    y = jnp.where(me == (owner + 1) % NDEV, own, 0.0)
    lane = lanes((H, WIN))
    known = jnp.where(
        lane == 2 * me,
        offsets[0].astype(F32),
        jnp.where(lane == 2 * me + 1, offsets[1].astype(F32), 0.0),
    )
    for i in range(GROUP):
        share[i, 0:4] = x
        share[i, 4:8] = y
        share[i, 8] = known
    halo[0:4] = own
    halo[4:8] = noise[0]


def relay_kernel(got, share):
    total = got[0]
    for i in range(1, GROUP):
        total = total + got[i]
    for i in range(GROUP):
        share[i] = total


def weights_of(refs):
    names = ("w_in", "w_mid", "w_out", "w_in_t", "w_mid_t", "w_out_t")
    return dict(zip(names, refs))


def first_kernel(
    me_ref, anchors, offsets, w_feat, latent, noise, halo, shared,
    w_in, w_mid, w_out, w_in_t, w_mid_t, w_out_t, embed,
    share, own_out, spill_out, inverse, *scratch,
):
    weights = weights_of((w_in, w_mid, w_out, w_in_t, w_mid_t, w_out_t))
    me = me_ref[0]
    total = shared[0]
    for i in range(1, GROUP):
        total = total + shared[i]
    table = total[8]
    lane = lanes((H, WIN))

    def offset_of(window):
        picked = jnp.where(lane == window, table, 0.0)[0:1]
        return jnp.sum(picked).astype(jnp.int32)

    starts = (offsets[0], STRIDE + offsets[1])
    anchor_at = (anchors[0] % 2) * STRIDE + offset_of(anchors[0])
    anchor = cut(total[0:4], total[4:8], anchor_at)
    plain_own, plain_spill, steep_own, steep_spill, square = step(
        0, latent[...], halo[0:4], starts, anchor, weights, embed, w_feat, scratch
    )
    spread = plan(0)[-1]

    def covered(windows):
        count = jnp.zeros((H, WIN), F32)
        for begin in windows:
            count = count + jnp.where((lane >= begin) & (lane < begin + WIN), 1.0, 0.0)
        return 1.0 / count

    left, right = 2 * me + NWIN - 2, 2 * me + 2
    before = (
        offset_of(left % NWIN) - WIN,
        offset_of((left + 1) % NWIN) - STRIDE,
    )
    after = (offset_of(right % NWIN), STRIDE + offset_of((right + 1) % NWIN))
    inverse_own = covered(before + starts)
    inverse_next = covered((starts[0] - WIN, starts[1] - WIN) + after)
    inverse[0] = inverse_own
    inverse[1] = inverse_next
    own_out[0:4] = plain_own
    own_out[4:8] = steep_own
    spill_out[0:4] = plain_spill
    spill_out[4:8] = steep_spill

    owner = anchors[1] // 2
    next_at = (anchors[1] % 2) * STRIDE + offset_of(anchors[1])
    here, ahead, behind = (
        me == owner, me == (owner + 1) % NDEV, me == (owner + NDEV - 1) % NDEV
    )

    def portion(own, spill):
        x = jnp.where(here, own, jnp.where(behind, spill, 0.0))
        y = jnp.where(here, spill, jnp.where(ahead, own, 0.0))
        return cut(x, y, next_at)

    plain_part = portion(
        plain_own * inverse_own + spread * noise[0], plain_spill * inverse_next
    )
    steep_part = portion(steep_own * inverse_own, steep_spill * inverse_next)
    for i in range(GROUP):
        share[i, 0:4] = plain_part
        share[i, 4:8] = steep_part
        share[i, 8] = square


def second_kernel(
    offsets, w_feat, guidance, noise, halo, shared, own_in, spill_in, spill_left, own_right, inverse,
    w_in, w_mid, w_out, w_in_t, w_mid_t, w_out_t, embed,
    own_out, spill_out, square_out, *scratch,
):
    weights = weights_of((w_in, w_mid, w_out, w_in_t, w_mid_t, w_out_t))
    total = shared[0]
    for i in range(1, GROUP):
        total = total + shared[i]
    scale = scale_of(jnp.sum(total[8]), guidance)
    spread = plan(0)[-1]
    anchor = total[0:4] + scale * total[4:8]
    own = own_in[...] + spill_left[...]
    beyond = spill_in[...] + own_right[...]
    first = (own[0:4] + scale * own[4:8]) * inverse[0] + spread * noise[0]
    second = (beyond[0:4] + scale * beyond[4:8]) * inverse[1] + spread * halo[4:8]
    starts = (offsets[0], STRIDE + offsets[1])
    plain_own, plain_spill, steep_own, steep_spill, square = step(
        1, first, second, starts, anchor, weights, embed, w_feat, scratch
    )
    own_out[0:4] = plain_own
    own_out[4:8] = steep_own
    spill_out[0:4] = plain_spill
    spill_out[4:8] = steep_spill
    row = jnp.sum(square, axis=0, keepdims=True)
    square_out[...] = jnp.broadcast_to(row[None], (NDEV, 1, WIN))


def closing_kernel(guidance, squares, own_in, spill_left, inverse, noise, out):
    scale = scale_of(jnp.sum(squares[...]), guidance)
    own = own_in[...] + spill_left[...]
    spread = plan(1)[-1]
    out[...] = (own[0:4] + scale * own[4:8]) * inverse[0] + spread * noise[1]


def call(kernel, shapes, n_scalars, *args, scratch=(), megabytes=4):
    in_specs = [
        pl.BlockSpec(memory_space=pltpu.SMEM if i < n_scalars else pltpu.VMEM)
        for i in range(len(args))
    ]
    return pl.pallas_call(
        kernel,
        out_shape=[jax.ShapeDtypeStruct(shape, F32) for shape in shapes],
        in_specs=in_specs,
        out_specs=[pl.BlockSpec(memory_space=pltpu.VMEM) for _ in shapes],
        scratch_shapes=scratch,
        compiler_params=pltpu.CompilerParams(vmem_limit_bytes=megabytes << 20),
    )(*args)


def scratches():
    return [pltpu.VMEM((8 * TAPS, WIN), F32)] * 3 + [pltpu.VMEM((HID, 2 * FIELD), F32)] * 2


def exchanged(shares, axes):
    return lax.all_to_all(shares, axes, split_axis=0, concat_axis=0, tiled=True)


def passed_along(shard, by):
    return lax.ppermute(shard, WA, [(i, (i + by) % NDEV) for i in range(NDEV)])


def local(latent, noise, offsets, anchors, guidance, w_in, w_mid, w_out, t_embed, w_feat):
    me = lax.axis_index(WA).astype(jnp.int32).reshape(1)
    features = w_feat.reshape(-1)
    weights = (w_in, w_mid, w_out, w_in.T, w_mid.T, w_out.T, t_embed.T)
    blocks, group = (8, H, WIN), (GROUP, 9, H, WIN)

    share, halo = call(opening_kernel, (group, blocks), 3, me, anchors, offsets, latent, noise)
    halo = passed_along(halo, -1)
    share = exchanged(share, NEAR)
    (share,) = call(relay_kernel, (group,), 0, share)
    share = exchanged(share, FAR)

    share, own, spill, inverse = call(
        first_kernel, (group, blocks, blocks, (2, H, WIN)), 4,
        me, anchors, offsets, features, latent, noise, halo, share, *weights,
        scratch=scratches(), megabytes=24,
    )
    spill_left = passed_along(spill, 1)
    own_right = passed_along(own, -1)
    share = exchanged(share, NEAR)
    (share,) = call(relay_kernel, (group,), 0, share)
    share = exchanged(share, FAR)

    own, spill, squares = call(
        second_kernel, (blocks, blocks, (NDEV, 1, WIN)), 3,
        offsets, features, guidance, noise, halo, share, own, spill, spill_left, own_right,
        inverse, *weights,
        scratch=scratches(), megabytes=24,
    )
    spill_left = passed_along(spill, 1)
    squares = exchanged(squares, WA)
    (out,) = call(
        closing_kernel, ((C, H, WIN),), 1, guidance, squares, own, spill_left, inverse, noise
    )
    return out


def solution(mesh):
    finer = Mesh(mesh.devices.reshape(2, 4, 8, mesh.shape["ba"]), ("wa_0", "wa_1", "wa_2", "ba"))
    placed = (P("ba", None, WA), P(None, "ba", None, WA), P(WA), P(), P(), P(), P(), P(), P(), P())
    return jax.shard_map(
        local, mesh=finer, in_specs=placed, out_specs=P("ba", None, WA), check_vma=False
    )
```

```python
import math

import jax
import jax.numpy as jnp
from jax import lax
from jax.experimental import pallas as pl
from jax.experimental.pallas import tpu as pltpu
from jax.sharding import Mesh
from jax.sharding import PartitionSpec as P

C = 4
H = 8
HID = 320
FEAT = 64
WIN = 128
STRIDE = 64
NDEV = 64
NWIN = 128
TAPS = 9 * C
FIELD = H * WIN
OWN = 2
PER_TURN = 16
WA = ("wa_0", "wa_1", "wa_2")
NEAR = "wa_2"
FAR = ("wa_0", "wa_1")
GROUP = 8

TAP_SHIFTS = ((-1, -1), (-1, 0), (-1, 1), (0, -1), (0, 0), (0, 1), (1, -1), (1, 0), (1, 1))
CUMULATIVE_ALPHA = (0.35, 0.55, 0.72, 0.85, 0.93)
STABILITY = 1e-06
ELEMENTS = float(NWIN * C * H * WIN)
F32 = jnp.float32
BF16 = jnp.bfloat16


def plan(number):
    current = CUMULATIVE_ALPHA[number]
    following = CUMULATIVE_ALPHA[number + 1]
    spread = 0.3 * math.sqrt(1.0 - following)
    return (
        math.sqrt(current),
        math.sqrt(1.0 - current),
        math.sqrt(following),
        math.sqrt(1.0 - following - spread * spread),
        spread,
    )


def lanes(shape=(C, H, WIN)):
    return lax.broadcasted_iota(jnp.int32, shape, len(shape) - 1)


def shift_rows(x, by):
    if by == 0:
        return x
    row = lax.broadcasted_iota(jnp.int32, x.shape, 1)
    inside = row >= 1 if by < 0 else row < H - 1
    return jnp.where(inside, pltpu.roll(x, (-by) % H, 1), 0.0)


def shift_lanes(x, by):
    if by == 0:
        return x
    lane = lanes(x.shape)
    inside = lane >= 1 if by < 0 else lane < WIN - 1
    return jnp.where(inside, pltpu.roll(x, (-by) % WIN, 2), 0.0)


def spread_taps(x, sign, tall):
    moved = {by: shift_lanes(x, sign * by) for by in (-1, 0, 1)}
    for k, (down, right) in enumerate(TAP_SHIFTS):
        tall[32 * k : 32 * (k + 1), :] = shift_rows(moved[right], sign * down).reshape(32, WIN)
    rows = [tall[pl.ds(h, TAPS, stride=H), :] for h in range(H)]
    return jnp.concatenate(rows, axis=1).astype(BF16)


def store_taps(tall, values):
    for h in range(H):
        tall[pl.ds(h, TAPS, stride=H), :] = values[:, WIN * h : WIN * (h + 1)]


def gather_taps(tall, sign):
    total = None
    for right in (-1, 0, 1):
        part = None
        for k, (down, across) in enumerate(TAP_SHIFTS):
            if across == right:
                piece = tall[32 * k : 32 * (k + 1), :].reshape(C, H, WIN)
                piece = shift_rows(piece, sign * down)
                part = piece if part is None else part + piece
        part = shift_lanes(part, sign * right)
        total = part if total is None else total + part
    return total


def silu_and_slope(half):
    p = 1.0 + jnp.tanh(half)
    return half * p, p * (1.0 + half * (2.0 - p))


def silu(half):
    return half * (1.0 + jnp.tanh(half))


def dot(a, b):
    return lax.dot_general(a, b, (((1,), (0,)), ((), ())), preferred_element_type=F32)


def predict(windows, weights, embed, talls, slopes):
    shared = range(len(windows))
    halves = [
        (dot(weights["w_in"][...], spread_taps(windows[i], 1, talls[i])) + embed).astype(BF16)
        for i in shared
    ]

    def activated(values, kept, i):
        if i >= OWN:
            return silu(values)
        value, kept[:, i * FIELD : (i + 1) * FIELD] = silu_and_slope(values)
        return value

    middles = [
        dot(weights["w_mid"][...], activated(halves[i], slopes[0], i)).astype(BF16) for i in shared
    ]
    for i in shared:
        joined = (halves[i] + halves[i]) + activated(middles[i], slopes[1], i)
        store_taps(talls[i], dot(weights["w_out"][...], joined))
    return [gather_taps(tall, 1) for tall in talls]


def pull_back(cotangents, weights, talls, slopes):
    own = range(OWN)
    at = [slice(i * FIELD, (i + 1) * FIELD) for i in own]
    d_joined = [
        dot(weights["w_out_t"][...], spread_taps(cotangents[i], -1, talls[i])).astype(BF16)
        for i in own
    ]
    d_active = [
        dot(weights["w_mid_t"][...], d_joined[i] * slopes[1][:, at[i]]).astype(BF16) for i in own
    ]
    for i in own:
        d_hidden = d_joined[i] + d_active[i] * slopes[0][:, at[i]]
        store_taps(talls[i], dot(weights["w_in_t"][...], d_hidden))
    return [gather_taps(tall, -1) for tall in talls]


def percept_pull_back(cleans, anchor, w_feat):
    fields = [[0.5 * x[c] for c in range(C)] for x in (anchor, *cleans)]
    many = len(cleans)

    def some(turn, grads):
        grads = list(grads)
        for i in range(PER_TURN):
            f = turn * PER_TURN + i
            w = [w_feat[f * C + c] for c in range(C)]
            mixed = [(w[0] * x[0] + w[1] * x[1]) + (w[2] * x[2] + w[3] * x[3]) for x in fields]
            target = silu(mixed[0])
            for j in range(many):
                s, slope = silu_and_slope(mixed[1 + j])
                d = (s - target) * slope
                for c in range(C):
                    grads[j * C + c] = grads[j * C + c] + w[c] * d
        return tuple(grads)

    nothing = tuple(jnp.zeros((H, WIN), F32) for _ in range(C * many))
    grads = lax.fori_loop(0, FEAT // PER_TURN, some, nothing)
    return [jnp.stack(grads[C * j : C * (j + 1)]) * (0.5 / FEAT) for j in range(many)]


def cut(first, second, start):
    by = (WIN - start) % WIN
    return jnp.where(
        lanes() < WIN - start, pltpu.roll(first, by, 2), pltpu.roll(second, by, 2)
    )


def place(pieces, starts):
    own, spill = 0.0, 0.0
    for piece, start in zip(pieces, starts):
        moved = pltpu.roll(piece, start, 2)
        inside = lanes() >= start
        own = own + jnp.where(inside, moved, 0.0)
        spill = spill + jnp.where(inside, 0.0, moved)
    return own, spill


def step(number, first, second, starts, anchor, weights, embed_ref, w_feat, scratch):
    now_a, now_s, next_a, direction, _ = plan(number)
    talls, slopes = scratch[:3], scratch[3:5]
    embed = embed_ref[:, number : number + 1]
    windows = [cut(first, second, start) for start in starts]
    every = windows + [anchor]
    predicted = predict(every, weights, embed, talls, slopes)
    cleans = [(w - now_s * p) * (1.0 / now_a) for w, p in zip(every, predicted)]
    d_cleans = percept_pull_back(cleans[:OWN], cleans[OWN], w_feat)
    pulled = pull_back([d * (-now_s / now_a) for d in d_cleans], weights, talls[:OWN], slopes)
    gradients = [d * (1.0 / now_a) + g for d, g in zip(d_cleans, pulled)]
    square = sum(jnp.sum(g * g, axis=0) for g in gradients)
    plain = [
        (next_a / now_a) * (w - now_s * p) + direction * p for w, p in zip(windows, predicted)
    ]
    plain_own, plain_spill = place(plain, starts)
    steep_own, steep_spill = place([g * (-next_a / now_a) for g in gradients], starts)
    return plain_own, plain_spill, steep_own, steep_spill, square


def scale_of(total, guidance):
    return guidance[0] * lax.rsqrt(jnp.full((1, 1, 1), total) * (1.0 / ELEMENTS) + STABILITY)


def opening_kernel(me_ref, offsets, latent, share):
    me = me_ref[0]
    own = latent[...]
    lane = lanes((H, WIN))
    known = jnp.where(
        lane == 2 * me,
        offsets[0].astype(F32),
        jnp.where(lane == 2 * me + 1, offsets[1].astype(F32), 0.0),
    )
    for i in range(GROUP):
        share[i, 0:4] = own
        share[i, 4] = known


def opening_relay_kernel(me_ref, anchors, got, share, beside):
    row, place_in_row = me_ref[0] // GROUP, me_ref[0] % GROUP
    owner = anchors[0] // 2

    def block_of(device):
        return jnp.where(device // GROUP == row, got[device % GROUP, 0:4], 0.0)

    x, y = block_of(owner), block_of((owner + 1) % NDEV)
    right = got[(place_in_row + 1) % GROUP, 0:4]
    known = got[0, 4]
    for i in range(1, GROUP):
        known = known + got[i, 4]
    beside[...] = right
    for i in range(GROUP):
        share[i, 0:4] = x
        share[i, 4:8] = y
        share[i, 8:12] = right
        share[i, 12] = known


def relay_kernel(got, share):
    total = got[0]
    for i in range(1, GROUP):
        total = total + got[i]
    for i in range(GROUP):
        share[i] = total


def weights_of(refs):
    names = ("w_in", "w_mid", "w_out", "w_in_t", "w_mid_t", "w_out_t")
    return dict(zip(names, refs))


def first_kernel(
    me_ref, anchors, offsets, w_feat, latent, noise, beside, shared,
    w_in, w_mid, w_out, w_in_t, w_mid_t, w_out_t, embed,
    share, own_out, spill_out, inverse, *scratch,
):
    weights = weights_of((w_in, w_mid, w_out, w_in_t, w_mid_t, w_out_t))
    me = me_ref[0]

    def summed(at):
        total = shared[0, at]
        for i in range(1, GROUP):
            total = total + shared[i, at]
        return total

    table = summed(12)
    lane = lanes((H, WIN))

    def offset_of(window):
        picked = jnp.where(lane == window, table, 0.0)[0:1]
        return jnp.sum(picked).astype(jnp.int32)

    starts = (offsets[0], STRIDE + offsets[1])
    anchor_at = (anchors[0] % 2) * STRIDE + offset_of(anchors[0])
    anchor = cut(summed(pl.ds(0, 4)), summed(pl.ds(4, 4)), anchor_at)
    across = shared[(me // GROUP + 1) % GROUP, 8:12]
    following = jnp.where(me % GROUP == GROUP - 1, across, beside[...])
    plain_own, plain_spill, steep_own, steep_spill, square = step(
        0, latent[...], following, starts, anchor, weights, embed, w_feat, scratch
    )
    spread = plan(0)[-1]

    def covered(windows):
        count = jnp.zeros((H, WIN), F32)
        for begin in windows:
            count = count + jnp.where((lane >= begin) & (lane < begin + WIN), 1.0, 0.0)
        return 1.0 / count

    left, right = 2 * me + NWIN - 2, 2 * me + 2
    before = (
        offset_of(left % NWIN) - WIN,
        offset_of((left + 1) % NWIN) - STRIDE,
    )
    after = (offset_of(right % NWIN), STRIDE + offset_of((right + 1) % NWIN))
    inverse_own = covered(before + starts)
    inverse_next = covered((starts[0] - WIN, starts[1] - WIN) + after)
    inverse[0] = inverse_own
    inverse[1] = inverse_next
    plain_own = plain_own * inverse_own + spread * noise[0]
    steep_own = steep_own * inverse_own
    plain_spill = plain_spill * inverse_next
    steep_spill = steep_spill * inverse_next
    own_out[0:4] = plain_own
    own_out[4:8] = steep_own
    spill_out[0:4] = plain_spill
    spill_out[4:8] = steep_spill

    owner = anchors[1] // 2
    next_at = (anchors[1] % 2) * STRIDE + offset_of(anchors[1])
    here, ahead, behind = (
        me == owner, me == (owner + 1) % NDEV, me == (owner + NDEV - 1) % NDEV
    )

    def portion(own, spill):
        x = jnp.where(here, own, jnp.where(behind, spill, 0.0))
        y = jnp.where(here, spill, jnp.where(ahead, own, 0.0))
        return cut(x, y, next_at)

    plain_part = portion(plain_own, plain_spill)
    steep_part = portion(steep_own, steep_spill)
    for i in range(GROUP):
        share[i, 0:4] = plain_part
        share[i, 4:8] = steep_part
        share[i, 8] = square


def second_kernel(
    offsets, w_feat, guidance, noise, shared, own_in, spill_in, spill_left, own_right, inverse,
    w_in, w_mid, w_out, w_in_t, w_mid_t, w_out_t, embed,
    own_out, spill_out, square_out, *scratch,
):
    weights = weights_of((w_in, w_mid, w_out, w_in_t, w_mid_t, w_out_t))
    total = shared[0]
    for i in range(1, GROUP):
        total = total + shared[i]
    scale = scale_of(jnp.sum(total[8]), guidance)
    spread = plan(1)[-1]
    anchor = total[0:4] + scale * total[4:8]
    own = own_in[...] + spill_left[...]
    beyond = spill_in[...] + own_right[...]
    first = own[0:4] + scale * own[4:8]
    second = beyond[0:4] + scale * beyond[4:8]
    starts = (offsets[0], STRIDE + offsets[1])
    plain_own, plain_spill, steep_own, steep_spill, square = step(
        1, first, second, starts, anchor, weights, embed, w_feat, scratch
    )
    own_out[0:4] = plain_own * inverse[0] + spread * noise[1]
    own_out[4:8] = steep_own * inverse[0]
    spill_out[0:4] = plain_spill * inverse[1]
    spill_out[4:8] = steep_spill * inverse[1]
    row = jnp.sum(square, axis=0, keepdims=True)
    square_out[...] = jnp.broadcast_to(row[None], (NDEV, 1, WIN))


def closing_kernel(guidance, squares, own_in, spill_left, out):
    scale = scale_of(jnp.sum(squares[...]), guidance)
    own = own_in[...] + spill_left[...]
    out[...] = own[0:4] + scale * own[4:8]


def call(kernel, shapes, n_scalars, *args, scratch=(), megabytes=4):
    in_specs = [
        pl.BlockSpec(memory_space=pltpu.SMEM if i < n_scalars else pltpu.VMEM)
        for i in range(len(args))
    ]
    return pl.pallas_call(
        kernel,
        out_shape=[jax.ShapeDtypeStruct(shape, F32) for shape in shapes],
        in_specs=in_specs,
        out_specs=[pl.BlockSpec(memory_space=pltpu.VMEM) for _ in shapes],
        scratch_shapes=scratch,
        compiler_params=pltpu.CompilerParams(vmem_limit_bytes=megabytes << 20),
    )(*args)


def scratches():
    return (
        [pltpu.VMEM((8 * TAPS, WIN), F32)] * (OWN + 1)
        + [pltpu.VMEM((HID, OWN * FIELD), BF16)] * 2
    )


def exchanged(shares, axes):
    return lax.all_to_all(shares, axes, split_axis=0, concat_axis=0, tiled=True)


def passed_along(shard, by):
    return lax.ppermute(shard, WA, [(i, (i + by) % NDEV) for i in range(NDEV)])


def local(latent, noise, offsets, anchors, guidance, w_in, w_mid, w_out, t_embed, w_feat):
    me = lax.axis_index(WA).astype(jnp.int32).reshape(1)
    features = w_feat.reshape(-1)
    weights = (
        w_in * 0.5, w_mid * 0.5, w_out, w_in.T, w_mid.T * 0.25, w_out.T, t_embed.T * 0.5
    )
    blocks, group = (8, H, WIN), (GROUP, 9, H, WIN)

    (share,) = call(opening_kernel, ((GROUP, 5, H, WIN),), 2, me, offsets, latent)
    share = exchanged(share, NEAR)
    share, beside = call(
        opening_relay_kernel, ((GROUP, 13, H, WIN), (C, H, WIN)), 2, me, anchors, share
    )
    share = exchanged(share, FAR)

    share, own, spill, inverse = call(
        first_kernel, (group, blocks, blocks, (2, H, WIN)), 4,
        me, anchors, offsets, features, latent, noise, beside, share, *weights,
        scratch=scratches(), megabytes=32,
    )
    spill_left = passed_along(spill, 1)
    own_right = passed_along(own, -1)
    share = exchanged(share, NEAR)
    (share,) = call(relay_kernel, (group,), 0, share)
    share = exchanged(share, FAR)

    own, spill, squares = call(
        second_kernel, (blocks, blocks, (NDEV, 1, WIN)), 3,
        offsets, features, guidance, noise, share, own, spill, spill_left, own_right,
        inverse, *weights,
        scratch=scratches(), megabytes=32,
    )
    spill_left = passed_along(spill, 1)
    squares = exchanged(squares, WA)
    (out,) = call(closing_kernel, ((C, H, WIN),), 1, guidance, squares, own, spill_left)
    return out


def solution(mesh):
    finer = Mesh(mesh.devices.reshape(2, 4, 8, mesh.shape["ba"]), ("wa_0", "wa_1", "wa_2", "ba"))
    placed = (P("ba", None, WA), P(None, "ba", None, WA), P(WA), P(), P(), P(), P(), P(), P(), P())
    return jax.shard_map(
        local, mesh=finer, in_specs=placed, out_specs=P("ba", None, WA), check_vma=False
    )
```

```python
import math

import jax
import jax.numpy as jnp
from jax import lax
from jax.experimental import pallas as pl
from jax.experimental.pallas import tpu as pltpu
from jax.sharding import Mesh
from jax.sharding import PartitionSpec as P

C = 4
H = 8
HID = 320
FEAT = 64
WIN = 128
STRIDE = 64
NDEV = 64
NWIN = 128
TAPS = 9 * C
FIELD = H * WIN
OWN = 2
PER_TURN = 16
WA = ("wa_0", "wa_1", "wa_2")
NEAR = "wa_2"
FAR = ("wa_0", "wa_1")
GROUP = 8

TAP_SHIFTS = ((-1, -1), (-1, 0), (-1, 1), (0, -1), (0, 0), (0, 1), (1, -1), (1, 0), (1, 1))
CUMULATIVE_ALPHA = (0.35, 0.55, 0.72, 0.85, 0.93)
STABILITY = 1e-06
ELEMENTS = float(NWIN * C * H * WIN)
F32 = jnp.float32
BF16 = jnp.bfloat16


def plan(number):
    current = CUMULATIVE_ALPHA[number]
    following = CUMULATIVE_ALPHA[number + 1]
    spread = 0.3 * math.sqrt(1.0 - following)
    return (
        math.sqrt(current),
        math.sqrt(1.0 - current),
        math.sqrt(following),
        math.sqrt(1.0 - following - spread * spread),
        spread,
    )


def lanes(shape=(C, H, WIN)):
    return lax.broadcasted_iota(jnp.int32, shape, len(shape) - 1)


def shift_rows(x, by):
    if by == 0:
        return x
    row = lax.broadcasted_iota(jnp.int32, x.shape, 1)
    inside = row >= 1 if by < 0 else row < H - 1
    return jnp.where(inside, pltpu.roll(x, (-by) % H, 1), 0.0)


def shift_lanes(x, by):
    if by == 0:
        return x
    lane = lanes(x.shape)
    inside = lane >= 1 if by < 0 else lane < WIN - 1
    return jnp.where(inside, pltpu.roll(x, (-by) % WIN, 2), 0.0)


def spread_taps(x, sign, tall):
    moved = {by: shift_lanes(x, sign * by) for by in (-1, 0, 1)}
    for k, (down, right) in enumerate(TAP_SHIFTS):
        tall[32 * k : 32 * (k + 1), :] = shift_rows(moved[right], sign * down).reshape(32, WIN)
    rows = [tall[pl.ds(h, TAPS, stride=H), :] for h in range(H)]
    return jnp.concatenate(rows, axis=1).astype(BF16)


def store_taps(tall, values):
    for h in range(H):
        tall[pl.ds(h, TAPS, stride=H), :] = values[:, WIN * h : WIN * (h + 1)]


def gather_taps(tall, sign):
    total = None
    for right in (-1, 0, 1):
        part = None
        for k, (down, across) in enumerate(TAP_SHIFTS):
            if across == right:
                piece = tall[32 * k : 32 * (k + 1), :].reshape(C, H, WIN)
                piece = shift_rows(piece, sign * down)
                part = piece if part is None else part + piece
        part = shift_lanes(part, sign * right)
        total = part if total is None else total + part
    return total


def silu_and_slope(half):
    p = 1.0 + jnp.tanh(half)
    return half * p, p * (1.0 + half * (2.0 - p))


def silu(half):
    return half * (1.0 + jnp.tanh(half))


def dot(a, b):
    return lax.dot_general(a, b, (((1,), (0,)), ((), ())), preferred_element_type=F32)


def predict(windows, weights, embed, talls, slopes):
    shared = range(len(windows))
    halves = [
        (dot(weights["w_in"][...], spread_taps(windows[i], 1, talls[i])) + embed).astype(BF16)
        for i in shared
    ]

    def activated(values, kept, i):
        if i >= OWN:
            return silu(values)
        value, kept[:, i * FIELD : (i + 1) * FIELD] = silu_and_slope(values)
        return value

    middles = [
        dot(weights["w_mid"][...], activated(halves[i], slopes[0], i)).astype(BF16) for i in shared
    ]
    for i in shared:
        joined = (halves[i] + halves[i]) + activated(middles[i], slopes[1], i)
        store_taps(talls[i], dot(weights["w_out"][...], joined))
    return [gather_taps(tall, 1) for tall in talls]


def pull_back(cotangents, weights, talls, slopes):
    own = range(OWN)
    at = [slice(i * FIELD, (i + 1) * FIELD) for i in own]
    d_joined = [
        dot(weights["w_out_t"][...], spread_taps(cotangents[i], -1, talls[i])).astype(BF16)
        for i in own
    ]
    d_active = [
        dot(weights["w_mid_t"][...], d_joined[i] * slopes[1][:, at[i]]).astype(BF16) for i in own
    ]
    for i in own:
        d_hidden = d_joined[i] + d_active[i] * slopes[0][:, at[i]]
        store_taps(talls[i], dot(weights["w_in_t"][...], d_hidden))
    return [gather_taps(tall, -1) for tall in talls]


def percept_pull_back(cleans, anchor, w_feat):
    fields = [[0.5 * x[c] for c in range(C)] for x in (anchor, *cleans)]
    many = len(cleans)

    def some(turn, grads):
        grads = list(grads)
        for i in range(PER_TURN):
            f = turn * PER_TURN + i
            w = [w_feat[c, f] for c in range(C)]
            mixed = [(w[0] * x[0] + w[1] * x[1]) + (w[2] * x[2] + w[3] * x[3]) for x in fields]
            target = silu(mixed[0])
            for j in range(many):
                s, slope = silu_and_slope(mixed[1 + j])
                d = (s - target) * slope
                for c in range(C):
                    grads[j * C + c] = grads[j * C + c] + w[c] * d
        return tuple(grads)

    nothing = tuple(jnp.zeros((H, WIN), F32) for _ in range(C * many))
    grads = lax.fori_loop(0, FEAT // PER_TURN, some, nothing)
    return [jnp.stack(grads[C * j : C * (j + 1)]) * (0.5 / FEAT) for j in range(many)]


def cut(first, second, start):
    by = (WIN - start) & (WIN - 1)
    return jnp.where(
        lanes() < WIN - start, pltpu.roll(first, by, 2), pltpu.roll(second, by, 2)
    )


def place(pieces, starts):
    own, spill = 0.0, 0.0
    for piece, start in zip(pieces, starts):
        moved = pltpu.roll(piece, start, 2)
        inside = lanes() >= start
        own = own + jnp.where(inside, moved, 0.0)
        spill = spill + jnp.where(inside, 0.0, moved)
    return own, spill


def step(number, first, second, starts, anchor, weights, embed_ref, w_feat, scratch):
    now_a, now_s, next_a, direction, _ = plan(number)
    talls, slopes = scratch[:3], scratch[3:5]
    embed = jnp.concatenate([embed_ref[number]] * (FIELD // WIN), axis=1)
    windows = [cut(first, second, start) for start in starts]
    every = windows + [anchor]
    predicted = predict(every, weights, embed, talls, slopes)
    cleans = [(w - now_s * p) * (1.0 / now_a) for w, p in zip(every, predicted)]
    feat_copy, feat_held = w_feat
    feat_copy.wait()
    d_cleans = percept_pull_back(cleans[:OWN], cleans[OWN], feat_held)
    pulled = pull_back([d * (-now_s / now_a) for d in d_cleans], weights, talls[:OWN], slopes)
    gradients = [d * (1.0 / now_a) + g for d, g in zip(d_cleans, pulled)]
    square = sum(jnp.sum(g * g, axis=0) for g in gradients)
    plain = [
        (next_a / now_a) * (w - now_s * p) + direction * p for w, p in zip(windows, predicted)
    ]
    plain_own, plain_spill = place(plain, starts)
    steep_own, steep_spill = place([g * (-next_a / now_a) for g in gradients], starts)
    return plain_own, plain_spill, steep_own, steep_spill, square


def scale_of(total, guidance):
    return guidance[...] * lax.rsqrt(jnp.full((H, WIN), total) * (1.0 / ELEMENTS) + STABILITY)


def opening_kernel(
    guidance, offsets, latent, t_embed, share, strength, t_embed_held, held, shifts, arrived
):
    copies = [
        pltpu.make_async_copy(latent, held, arrived.at[0]),
        pltpu.make_async_copy(offsets, shifts, arrived.at[1]),
        pltpu.make_async_copy(t_embed, t_embed_held, arrived.at[2]),
    ]
    for copy in copies:
        copy.start()
    strength[...] = jnp.full((H, WIN), guidance[0])
    for copy in copies:
        copy.wait()
    own = held[...]
    lane = lanes((H, WIN))
    known = jnp.where(
        lane == 0, shifts[0].astype(F32), jnp.where(lane == 1, shifts[1].astype(F32), 0.0)
    )
    for i in range(GROUP):
        share[i, 0:4] = own
        share[i, 4] = known


def opening_relay_kernel(anchors, got, share, beside):
    row, column = lax.axis_index(FAR), lax.axis_index(NEAR)
    owner = anchors[0] >> 1

    def block_of(device):
        return jnp.where(device >> 3 == row, got[device & 7, 0:4], 0.0)

    x, y = block_of(owner), block_of((owner + 1) & (NDEV - 1))
    right = got[(column + 1) & 7, 0:4]
    known = got[0, 4]
    for i in range(1, GROUP):
        known = known + pltpu.roll(got[i, 4], 2 * i, 1)
    known = pltpu.roll(known, 2 * GROUP * row, 1)
    beside[...] = right
    for i in range(GROUP):
        share[i, 0:4] = x
        share[i, 4:8] = y
        share[i, 8:12] = right
        share[i, 12] = known


def relay_kernel(got, share):
    total = got[0]
    for i in range(1, GROUP):
        total = total + got[i]
    for i in range(GROUP):
        share[i] = total


def prepare(w_in_t, w_mid, w_out, t_embed, w_in, w_mid_half, w_mid_t, w_out_t, embed):
    def turned(values, factor):
        return (values.astype(F32).T * factor).astype(BF16)

    w_in[...] = turned(w_in_t[...], 0.5)
    w_mid_half[...] = (w_mid[...].astype(F32) * 0.5).astype(BF16)
    w_mid_t[...] = turned(w_mid[...], 0.25)
    w_out_t[...] = turned(w_out[...], 1.0)
    for number in range(2):
        row = jnp.broadcast_to(t_embed[number : number + 1, :] * 0.5, (WIN, HID))
        embed[number] = row.T


def fetches(noise, w_feat, scratch):
    noise_held, feat_held, arrived = scratch[:3]
    noise_copy = pltpu.make_async_copy(noise, noise_held, arrived.at[0])
    feat_copy = pltpu.make_async_copy(w_feat, feat_held, arrived.at[1])
    noise_copy.start()
    feat_copy.start()
    return noise_copy, feat_copy, noise_held, feat_held, scratch[3:]


def offset_in(table, window):
    row = table[0:1, :]
    return jnp.sum(jnp.where(lanes((1, WIN)) == window, row, 0.0)).astype(jnp.int32)


def weights_of(refs):
    names = ("w_in", "w_mid", "w_out", "w_in_t", "w_mid_t", "w_out_t")
    return dict(zip(names, refs))


def first_kernel(
    anchors, w_feat, noise, latent, beside, shared,
    w_in_t, w_mid, w_out, t_embed,
    share, own_out, spill_out, inverse, table_out, w_in, w_mid_half, w_mid_t, w_out_t, embed,
    *scratch,
):
    table_held, table_arrived, *scratch = scratch

    def summed(at):
        total = shared[0, at]
        for i in range(1, GROUP):
            total = total + shared[i, at]
        return total

    table_out[...] = summed(12)
    table_copy = pltpu.make_async_copy(table_out, table_held, table_arrived)
    table_copy.start()
    noise_copy, feat_copy, noise_held, feat_held, scratch = fetches(noise.at[0], w_feat, scratch)
    prepare(w_in_t, w_mid, w_out, t_embed, w_in, w_mid_half, w_mid_t, w_out_t, embed)
    weights = weights_of((w_in, w_mid_half, w_out, w_in_t, w_mid_t, w_out_t))
    me = lax.axis_index(WA)
    lane = lanes((H, WIN))
    table_copy.wait()

    def offset_of(window):
        return table_held[0, window].astype(jnp.int32)

    starts = (offset_of(2 * me), STRIDE + offset_of(2 * me + 1))
    anchor_at = (anchors[0] & 1) * STRIDE + offset_of(anchors[0])
    anchor = cut(summed(pl.ds(0, 4)), summed(pl.ds(4, 4)), anchor_at)
    across = shared[((me >> 3) + 1) & 7, 8:12]
    following = jnp.where(me & 7 == 7, across, beside[...])
    plain_own, plain_spill, steep_own, steep_spill, square = step(
        0, latent[...], following, starts, anchor, weights, embed, (feat_copy, feat_held), scratch
    )
    spread = plan(0)[-1]

    def covered(windows):
        count = jnp.zeros((H, WIN), F32)
        for begin in windows:
            count = count + jnp.where((lane >= begin) & (lane < begin + WIN), 1.0, 0.0)
        return 1.0 / count

    left, right = 2 * me + NWIN - 2, 2 * me + 2
    before = (
        offset_of(left & (NWIN - 1)) - WIN,
        offset_of((left + 1) & (NWIN - 1)) - STRIDE,
    )
    after = (offset_of(right & (NWIN - 1)), STRIDE + offset_of((right + 1) & (NWIN - 1)))
    inverse_own = covered(before + starts)
    inverse_next = covered((starts[0] - WIN, starts[1] - WIN) + after)
    inverse[0] = inverse_own
    inverse[1] = inverse_next
    noise_copy.wait()
    plain_own = plain_own * inverse_own + spread * noise_held[...]
    steep_own = steep_own * inverse_own
    plain_spill = plain_spill * inverse_next
    steep_spill = steep_spill * inverse_next
    own_out[0:4] = plain_own
    own_out[4:8] = steep_own
    spill_out[0:4] = plain_spill
    spill_out[4:8] = steep_spill

    owner = anchors[1] >> 1
    next_at = (anchors[1] & 1) * STRIDE + offset_of(anchors[1])
    here, ahead, behind = (
        me == owner, me == (owner + 1) & (NDEV - 1), me == (owner - 1) & (NDEV - 1)
    )

    def portion(own, spill):
        x = jnp.where(here, own, jnp.where(behind, spill, 0.0))
        y = jnp.where(here, spill, jnp.where(ahead, own, 0.0))
        return cut(x, y, next_at)

    plain_part = portion(plain_own, plain_spill)
    steep_part = portion(steep_own, steep_spill)
    for i in range(GROUP):
        share[i, 0:4] = plain_part
        share[i, 4:8] = steep_part
        share[i, 8] = square


def second_kernel(
    w_feat, noise, guidance, table, shared, own_in, spill_in, spill_left, own_right, inverse,
    w_in, w_mid, w_out, w_in_t, w_mid_t, w_out_t, embed,
    own_out, spill_out, square_out, *scratch,
):
    noise_copy, feat_copy, noise_held, feat_held, scratch = fetches(noise.at[1], w_feat, scratch)
    me = lax.axis_index(WA)
    starts = (offset_in(table, 2 * me), STRIDE + offset_in(table, 2 * me + 1))
    weights = weights_of((w_in, w_mid, w_out, w_in_t, w_mid_t, w_out_t))
    total = shared[0]
    for i in range(1, GROUP):
        total = total + shared[i]
    scale = scale_of(jnp.sum(total[8]), guidance)
    spread = plan(1)[-1]
    anchor = total[0:4] + scale * total[4:8]
    own = own_in[...] + spill_left[...]
    beyond = spill_in[...] + own_right[...]
    first = own[0:4] + scale * own[4:8]
    second = beyond[0:4] + scale * beyond[4:8]
    plain_own, plain_spill, steep_own, steep_spill, square = step(
        1, first, second, starts, anchor, weights, embed, (feat_copy, feat_held), scratch
    )
    noise_copy.wait()
    own_out[0:4] = plain_own * inverse[0] + spread * noise_held[...]
    own_out[4:8] = steep_own * inverse[0]
    spill_out[0:4] = plain_spill * inverse[1]
    spill_out[4:8] = steep_spill * inverse[1]
    row = jnp.sum(square, axis=0, keepdims=True)
    square_out[...] = jnp.broadcast_to(row[None], (NDEV, 1, WIN))


def closing_kernel(guidance, squares, own_in, spill_left, out):
    scale = scale_of(jnp.sum(squares[...]), guidance)
    own = own_in[...] + spill_left[...]
    out[...] = own[0:4] + scale * own[4:8]


def call(kernel, shapes, spaces, *args, scratch=(), megabytes=4, near=True):
    kinds = {"s": pltpu.SMEM, "h": pltpu.HBM, "v": pltpu.VMEM}
    in_specs = [
        pl.BlockSpec(memory_space=kinds[letter]) for letter in spaces.ljust(len(args), "v")
    ]
    args = [
        pltpu.with_memory_space_constraint(arg, pltpu.HBM) if letter == "h" else arg
        for arg, letter in zip(args, spaces.ljust(len(args), "v"))
    ]
    return pl.pallas_call(
        kernel,
        out_shape=[
            (pltpu.VMEM if near else jax.ShapeDtypeStruct)(
                *(shape if isinstance(shape[0], tuple) else (shape, F32))
            )
            for shape in shapes
        ],
        in_specs=in_specs,
        out_specs=[pl.BlockSpec(memory_space=pltpu.VMEM) for _ in shapes],
        scratch_shapes=scratch,
        compiler_params=pltpu.CompilerParams(vmem_limit_bytes=megabytes << 20),
    )(*args)


def scratches():
    return (
        [pltpu.VMEM((8 * TAPS, WIN), F32)] * (OWN + 1)
        + [pltpu.VMEM((HID, OWN * FIELD), BF16)] * 2
    )


def exchanged(shares, axes):
    return lax.all_to_all(shares, axes, split_axis=0, concat_axis=0, tiled=True)


def passed_along(shard, axes, by):
    length = lax.axis_size(axes)
    return lax.ppermute(shard, axes, [(i, (i + by) % length) for i in range(length)])


def local(latent, noise, offsets, anchors, guidance, w_in, w_mid, w_out, t_embed, w_feat):
    features = w_feat.T
    blocks = (8, H, WIN)
    tall, square = ((HID, TAPS), BF16), ((HID, HID), BF16)
    noise_place = [
        pltpu.VMEM((C, H, WIN), F32), pltpu.SMEM((C, FEAT), F32), pltpu.SemaphoreType.DMA((2,))
    ]

    share, strength, t_embed = call(
        opening_kernel, ((GROUP, 5, H, WIN), (H, WIN), (2, HID)), "shhh",
        guidance, offsets, latent, t_embed,
        scratch=[
            pltpu.VMEM((C, H, WIN), F32), pltpu.SMEM((2,), jnp.int32),
            pltpu.SemaphoreType.DMA((3,)),
        ],
    )
    share = exchanged(share, NEAR)
    share, beside = call(
        opening_relay_kernel, ((GROUP, 13, H, WIN), (C, H, WIN)), "s", anchors, share
    )
    share = exchanged(share, FAR)

    share, own, spill, inverse, table, w_in_half, w_mid_half, w_mid_t, w_out_t, embed = call(
        first_kernel,
        (
            (GROUP, 9, H, WIN), blocks, blocks, (2, H, WIN), (H, WIN),
            tall, square, square, tall, (2, HID, WIN),
        ),
        "shh",
        anchors, features, noise, latent, beside, share,
        w_in.T, w_mid, w_out, t_embed,
        scratch=[pltpu.SMEM((H, WIN), F32), pltpu.SemaphoreType.DMA] + noise_place + scratches(),
        megabytes=32,
    )
    spill_left = passed_along(spill, WA, 1)
    own_right = passed_along(own, WA, -1)
    share = exchanged(share, NEAR)
    (share,) = call(relay_kernel, ((GROUP, 9, H, WIN),), "", share)
    share = exchanged(share, FAR)

    own, spill, squares = call(
        second_kernel, (blocks, blocks, (NDEV, 1, WIN)), "hh",
        features, noise, strength, table, share, own, spill, spill_left, own_right,
        inverse, w_in_half, w_mid_half, w_out, w_in.T, w_mid_t, w_out_t, embed,
        scratch=noise_place + scratches(), megabytes=32,
    )
    spill_left = passed_along(spill, WA, 1)
    squares = exchanged(squares, WA)
    (out,) = call(
        closing_kernel, ((C, H, WIN),), "", strength, squares, own, spill_left, near=False
    )
    return out


def solution(mesh):
    finer = Mesh(mesh.devices.reshape(2, 4, 8, mesh.shape["ba"]), ("wa_0", "wa_1", "wa_2", "ba"))
    placed = (P("ba", None, WA), P(None, "ba", None, WA), P(WA), P(), P(), P(), P(), P(), P(), P())
    return jax.shard_map(
        local, mesh=finer, in_specs=placed, out_specs=P("ba", None, WA), check_vma=False
    )
```

```python
import math

import jax
import jax.numpy as jnp
from jax import lax
from jax.experimental import pallas as pl
from jax.experimental.pallas import tpu as pltpu
from jax.sharding import Mesh
from jax.sharding import PartitionSpec as P

C = 4
H = 8
HID = 320
FEAT = 64
WIN = 128
STRIDE = 64
NDEV = 64
NWIN = 128
TAPS = 9 * C
FIELD = H * WIN
OWN = 2
PER_TURN = 16
WA = ("wa_0", "wa_1", "wa_2")
NEAR = "wa_2"
FAR = ("wa_0", "wa_1")
GROUP = 8

TAP_SHIFTS = ((-1, -1), (-1, 0), (-1, 1), (0, -1), (0, 0), (0, 1), (1, -1), (1, 0), (1, 1))
CUMULATIVE_ALPHA = (0.35, 0.55, 0.72, 0.85, 0.93)
STABILITY = 1e-06
ELEMENTS = float(NWIN * C * H * WIN)
F32 = jnp.float32
BF16 = jnp.bfloat16


def plan(number):
    current = CUMULATIVE_ALPHA[number]
    following = CUMULATIVE_ALPHA[number + 1]
    spread = 0.3 * math.sqrt(1.0 - following)
    return (
        math.sqrt(current),
        math.sqrt(1.0 - current),
        math.sqrt(following),
        math.sqrt(1.0 - following - spread * spread),
        spread,
    )


def lanes(shape=(C, H, WIN)):
    return lax.broadcasted_iota(jnp.int32, shape, len(shape) - 1)


def shift_rows(x, by):
    if by == 0:
        return x
    row = lax.broadcasted_iota(jnp.int32, x.shape, 1)
    inside = row >= 1 if by < 0 else row < H - 1
    return jnp.where(inside, pltpu.roll(x, (-by) % H, 1), 0.0)


def shift_lanes(x, by):
    if by == 0:
        return x
    lane = lanes(x.shape)
    inside = lane >= 1 if by < 0 else lane < WIN - 1
    return jnp.where(inside, pltpu.roll(x, (-by) % WIN, 2), 0.0)


def spread_taps(x, sign, tall):
    moved = {by: shift_lanes(x, sign * by) for by in (-1, 0, 1)}
    for k, (down, right) in enumerate(TAP_SHIFTS):
        tall[32 * k : 32 * (k + 1), :] = shift_rows(moved[right], sign * down).reshape(32, WIN)
    rows = [tall[pl.ds(h, TAPS, stride=H), :] for h in range(H)]
    return jnp.concatenate(rows, axis=1).astype(BF16)


def store_taps(tall, values):
    for h in range(H):
        tall[pl.ds(h, TAPS, stride=H), :] = values[:, WIN * h : WIN * (h + 1)]


def gather_taps(tall, sign):
    total = None
    for right in (-1, 0, 1):
        part = None
        for k, (down, across) in enumerate(TAP_SHIFTS):
            if across == right:
                piece = tall[32 * k : 32 * (k + 1), :].reshape(C, H, WIN)
                piece = shift_rows(piece, sign * down)
                part = piece if part is None else part + piece
        part = shift_lanes(part, sign * right)
        total = part if total is None else total + part
    return total


def silu_and_slope(half):
    p = 1.0 + jnp.tanh(half)
    return half * p, p * (1.0 + half * (2.0 - p))


def silu(half):
    return half * (1.0 + jnp.tanh(half))


def dot(a, b):
    return lax.dot_general(a, b, (((1,), (0,)), ((), ())), preferred_element_type=F32)


def predict(windows, weights, embed, talls, slopes):
    shared = range(len(windows))
    halves = [
        (dot(weights["w_in"][...], spread_taps(windows[i], 1, talls[i])) + embed).astype(BF16)
        for i in shared
    ]

    def activated(values, kept, i):
        if i >= OWN:
            return silu(values)
        value, kept[:, i * FIELD : (i + 1) * FIELD] = silu_and_slope(values)
        return value

    middles = [
        dot(weights["w_mid"][...], activated(halves[i], slopes[0], i)).astype(BF16) for i in shared
    ]
    for i in shared:
        joined = (halves[i] + halves[i]) + activated(middles[i], slopes[1], i)
        store_taps(talls[i], dot(weights["w_out"][...], joined))
    return [gather_taps(tall, 1) for tall in talls]


def pull_back(cotangents, weights, talls, slopes):
    own = range(OWN)
    at = [slice(i * FIELD, (i + 1) * FIELD) for i in own]
    d_joined = [
        dot(weights["w_out_t"][...], spread_taps(cotangents[i], -1, talls[i])).astype(BF16)
        for i in own
    ]
    d_active = [
        dot(weights["w_mid_t"][...], d_joined[i] * slopes[1][:, at[i]]).astype(BF16) for i in own
    ]
    for i in own:
        d_hidden = d_joined[i] + d_active[i] * slopes[0][:, at[i]]
        store_taps(talls[i], dot(weights["w_in_t"][...], d_hidden))
    return [gather_taps(tall, -1) for tall in talls]


def percept_pull_back(cleans, anchor, w_feat):
    fields = [[0.5 * x[c] for c in range(C)] for x in (anchor, *cleans)]
    many = len(cleans)

    def some(turn, grads):
        grads = list(grads)
        for i in range(PER_TURN):
            f = turn * PER_TURN + i
            w = [w_feat[c, f] for c in range(C)]
            mixed = [(w[0] * x[0] + w[1] * x[1]) + (w[2] * x[2] + w[3] * x[3]) for x in fields]
            target = silu(mixed[0])
            for j in range(many):
                s, slope = silu_and_slope(mixed[1 + j])
                d = (s - target) * slope
                for c in range(C):
                    grads[j * C + c] = grads[j * C + c] + w[c] * d
        return tuple(grads)

    nothing = tuple(jnp.zeros((H, WIN), F32) for _ in range(C * many))
    grads = lax.fori_loop(0, FEAT // PER_TURN, some, nothing)
    return [jnp.stack(grads[C * j : C * (j + 1)]) * (0.5 / FEAT) for j in range(many)]


def cut(first, second, start):
    by = (WIN - start) & (WIN - 1)
    return jnp.where(
        lanes() < WIN - start, pltpu.roll(first, by, 2), pltpu.roll(second, by, 2)
    )


def place(pieces, starts):
    own, spill = 0.0, 0.0
    for piece, start in zip(pieces, starts):
        moved = pltpu.roll(piece, start, 2)
        inside = lanes() >= start
        own = own + jnp.where(inside, moved, 0.0)
        spill = spill + jnp.where(inside, 0.0, moved)
    return own, spill


def step(
    number, first, second, starts, anchor, weights, embed_ref, w_feat, scratch, prepare=lambda: None
):
    now_a, now_s, next_a, direction, _ = plan(number)
    talls, slopes = scratch[:3], scratch[3:5]
    embed = jnp.concatenate([embed_ref[number]] * (FIELD // WIN), axis=1)
    windows = [cut(first, second, start) for start in starts]
    every = windows + [anchor]
    predicted = predict(every, weights, embed, talls, slopes)
    cleans = [(w - now_s * p) * (1.0 / now_a) for w, p in zip(every, predicted)]
    prepare()
    feat_copy, feat_held = w_feat
    feat_copy.wait()
    d_cleans = percept_pull_back(cleans[:OWN], cleans[OWN], feat_held)
    pulled = pull_back([d * (-now_s / now_a) for d in d_cleans], weights, talls[:OWN], slopes)
    gradients = [d * (1.0 / now_a) + g for d, g in zip(d_cleans, pulled)]
    square = sum(jnp.sum(g * g, axis=0) for g in gradients)
    plain = [
        (next_a / now_a) * (w - now_s * p) + direction * p for w, p in zip(windows, predicted)
    ]
    plain_own, plain_spill = place(plain, starts)
    steep_own, steep_spill = place([g * (-next_a / now_a) for g in gradients], starts)
    return plain_own, plain_spill, steep_own, steep_spill, square


def scale_of(total, guidance):
    return guidance[...] * lax.rsqrt(jnp.full((H, WIN), total) * (1.0 / ELEMENTS) + STABILITY)


def opening_kernel(
    guidance, offsets, latent, t_embed, share, strength, t_embed_held, held, shifts, arrived
):
    copies = [
        pltpu.make_async_copy(latent, held, arrived.at[0]),
        pltpu.make_async_copy(offsets, shifts, arrived.at[1]),
        pltpu.make_async_copy(t_embed, t_embed_held, arrived.at[2]),
    ]
    for copy in copies:
        copy.start()
    strength[...] = jnp.full((H, WIN), guidance[0])
    for copy in copies:
        copy.wait()
    own = held[...]
    lane = lanes((H, WIN))
    known = jnp.where(
        lane == 0, shifts[0].astype(F32), jnp.where(lane == 1, shifts[1].astype(F32), 0.0)
    )
    for i in range(GROUP):
        share[i, 0:4] = own
        share[i, 4] = known


def opening_relay_kernel(anchors, got, share, beside):
    row, column = lax.axis_index(FAR), lax.axis_index(NEAR)
    owner = anchors[0] >> 1

    def block_of(device):
        return jnp.where(device >> 3 == row, got[device & 7, 0:4], 0.0)

    x, y = block_of(owner), block_of((owner + 1) & (NDEV - 1))
    right = got[(column + 1) & 7, 0:4]
    known = got[0, 4]
    for i in range(1, GROUP):
        known = known + pltpu.roll(got[i, 4], 2 * i, 1)
    known = pltpu.roll(known, 2 * GROUP * row, 1)
    beside[...] = right
    for i in range(GROUP):
        share[i, 0:4] = x
        share[i, 4:8] = y
        share[i, 8:12] = right
        share[i, 12] = known


def relay_kernel(got, share):
    total = got[0]
    for i in range(1, GROUP):
        total = total + got[i]
    for i in range(GROUP):
        share[i] = total


def turned(values, factor):
    return (values.astype(F32).T * factor).astype(BF16)


def column_of(row):
    return jnp.broadcast_to(row * 0.5, (WIN, HID)).T


def fetches(noise, w_feat, scratch):
    noise_held, feat_held, arrived = scratch[:3]
    noise_copy = pltpu.make_async_copy(noise, noise_held, arrived.at[0])
    feat_copy = pltpu.make_async_copy(w_feat, feat_held, arrived.at[1])
    noise_copy.start()
    feat_copy.start()
    return noise_copy, feat_copy, noise_held, feat_held, scratch[3:]


def offset_in(table, window):
    row = table[0:1, :]
    return jnp.sum(jnp.where(lanes((1, WIN)) == window, row, 0.0)).astype(jnp.int32)


def weights_of(refs):
    names = ("w_in", "w_mid", "w_out", "w_in_t", "w_mid_t", "w_out_t")
    return dict(zip(names, refs))


def first_kernel(
    anchors, w_feat, noise, latent, beside, shared,
    w_in_t, w_mid, w_out, t_embed,
    share, own_out, spill_out, inside, outside, inverse, table_out, w_in, w_mid_half, w_mid_t, w_out_t, embed,
    *scratch,
):
    table_held, table_arrived, *scratch = scratch

    def summed(at):
        total = shared[0, at]
        for i in range(1, GROUP):
            total = total + shared[i, at]
        return total

    table_out[...] = summed(12)
    table_copy = pltpu.make_async_copy(table_out, table_held, table_arrived)
    table_copy.start()
    noise_copy, feat_copy, noise_held, feat_held, scratch = fetches(noise.at[0], w_feat, scratch)
    w_in[...] = turned(w_in_t[...], 0.5)
    w_mid_half[...] = (w_mid[...].astype(F32) * 0.5).astype(BF16)
    embed[0] = column_of(t_embed[0:1, :])

    def prepare():
        w_mid_t[...] = turned(w_mid[...], 0.25)
        w_out_t[...] = turned(w_out[...], 1.0)
        embed[1] = column_of(t_embed[1:2, :])

    weights = weights_of((w_in, w_mid_half, w_out, w_in_t, w_mid_t, w_out_t))
    me = lax.axis_index(WA)
    lane = lanes((H, WIN))
    table_copy.wait()

    def offset_of(window):
        return table_held[0, window].astype(jnp.int32)

    starts = (offset_of(2 * me), STRIDE + offset_of(2 * me + 1))
    anchor_at = (anchors[0] & 1) * STRIDE + offset_of(anchors[0])
    anchor = cut(summed(pl.ds(0, 4)), summed(pl.ds(4, 4)), anchor_at)
    across = shared[((me >> 3) + 1) & 7, 8:12]
    following = jnp.where(me & 7 == 7, across, beside[...])
    plain_own, plain_spill, steep_own, steep_spill, square = step(
        0, latent[...], following, starts, anchor, weights, embed, (feat_copy, feat_held), scratch,
        prepare,
    )
    spread = plan(0)[-1]

    def covered(windows):
        count = jnp.zeros((H, WIN), F32)
        for begin in windows:
            count = count + jnp.where((lane >= begin) & (lane < begin + WIN), 1.0, 0.0)
        return 1.0 / count

    left, right = 2 * me + NWIN - 2, 2 * me + 2
    before = (
        offset_of(left & (NWIN - 1)) - WIN,
        offset_of((left + 1) & (NWIN - 1)) - STRIDE,
    )
    after = (offset_of(right & (NWIN - 1)), STRIDE + offset_of((right + 1) & (NWIN - 1)))
    inverse_own = covered(before + starts)
    inverse_next = covered((starts[0] - WIN, starts[1] - WIN) + after)
    inverse[0] = inverse_own
    inverse[1] = inverse_next
    noise_copy.wait()
    plain_own = plain_own * inverse_own + spread * noise_held[...]
    steep_own = steep_own * inverse_own
    plain_spill = plain_spill * inverse_next
    steep_spill = steep_spill * inverse_next
    own_out[0:4] = plain_own
    own_out[4:8] = steep_own
    spill_out[0:4] = plain_spill
    spill_out[4:8] = steep_spill
    odd = me & 1 == 1
    for at, own, spill in ((0, plain_own, plain_spill), (4, steep_own, steep_spill)):
        inside[at : at + 4] = jnp.where(odd, own, spill)
        outside[at : at + 4] = jnp.where(odd, spill, own)

    owner = anchors[1] >> 1
    next_at = (anchors[1] & 1) * STRIDE + offset_of(anchors[1])
    here, ahead, behind = (
        me == owner, me == (owner + 1) & (NDEV - 1), me == (owner - 1) & (NDEV - 1)
    )

    def portion(own, spill):
        x = jnp.where(here, own, jnp.where(behind, spill, 0.0))
        y = jnp.where(here, spill, jnp.where(ahead, own, 0.0))
        return cut(x, y, next_at)

    plain_part = portion(plain_own, plain_spill)
    steep_part = portion(steep_own, steep_spill)
    for i in range(GROUP):
        share[i, 0:4] = plain_part
        share[i, 4:8] = steep_part
        share[i, 8] = square


def second_kernel(
    w_feat, noise, guidance, table, shared, own_in, spill_in, inside, outside, inverse,
    w_in, w_mid, w_out, w_in_t, w_mid_t, w_out_t, embed,
    own_out, spill_out, square_out, *scratch,
):
    noise_copy, feat_copy, noise_held, feat_held, scratch = fetches(noise.at[1], w_feat, scratch)
    me = lax.axis_index(WA)
    starts = (offset_in(table, 2 * me), STRIDE + offset_in(table, 2 * me + 1))
    weights = weights_of((w_in, w_mid, w_out, w_in_t, w_mid_t, w_out_t))
    total = shared[0]
    for i in range(1, GROUP):
        total = total + shared[i]
    scale = scale_of(jnp.sum(total[8]), guidance)
    spread = plan(1)[-1]
    anchor = total[0:4] + scale * total[4:8]
    odd = me & 1 == 1
    own = own_in[...] + jnp.where(odd, inside[...], outside[...])
    beyond = spill_in[...] + jnp.where(odd, outside[...], inside[...])
    first = own[0:4] + scale * own[4:8]
    second = beyond[0:4] + scale * beyond[4:8]
    plain_own, plain_spill, steep_own, steep_spill, square = step(
        1, first, second, starts, anchor, weights, embed, (feat_copy, feat_held), scratch
    )
    noise_copy.wait()
    own_out[0:4] = plain_own * inverse[0] + spread * noise_held[...]
    own_out[4:8] = steep_own * inverse[0]
    spill_out[0:4] = plain_spill * inverse[1]
    spill_out[4:8] = steep_spill * inverse[1]
    row = jnp.sum(square, axis=0, keepdims=True)
    square_out[...] = jnp.broadcast_to(row[None], (NDEV, 1, WIN))


def closing_kernel(guidance, squares, own_in, spill_left, out):
    scale = scale_of(jnp.sum(squares[...]), guidance)
    own = own_in[...] + spill_left[...]
    out[...] = own[0:4] + scale * own[4:8]


def call(kernel, shapes, spaces, *args, scratch=(), megabytes=4, near=True):
    kinds = {"s": pltpu.SMEM, "h": pltpu.HBM, "v": pltpu.VMEM}
    in_specs = [
        pl.BlockSpec(memory_space=kinds[letter]) for letter in spaces.ljust(len(args), "v")
    ]
    args = [
        pltpu.with_memory_space_constraint(arg, pltpu.HBM) if letter == "h" else arg
        for arg, letter in zip(args, spaces.ljust(len(args), "v"))
    ]
    return pl.pallas_call(
        kernel,
        out_shape=[
            (pltpu.VMEM if near else jax.ShapeDtypeStruct)(
                *(shape if isinstance(shape[0], tuple) else (shape, F32))
            )
            for shape in shapes
        ],
        in_specs=in_specs,
        out_specs=[pl.BlockSpec(memory_space=pltpu.VMEM) for _ in shapes],
        scratch_shapes=scratch,
        compiler_params=pltpu.CompilerParams(vmem_limit_bytes=megabytes << 20),
    )(*args)


def scratches():
    return (
        [pltpu.VMEM((8 * TAPS, WIN), F32)] * (OWN + 1)
        + [pltpu.VMEM((HID, OWN * FIELD), BF16)] * 2
    )


def exchanged(shares, axes):
    return lax.all_to_all(shares, axes, split_axis=0, concat_axis=0, tiled=True)


def passed_along(shard, axes, by):
    length = lax.axis_size(axes)
    return lax.ppermute(shard, axes, [(i, (i + by) % length) for i in range(length)])


def swapped(shard, first):
    pairs = [((first + i) % NDEV, (first + (i ^ 1)) % NDEV) for i in range(NDEV)]
    return lax.ppermute(shard, WA, pairs)


def local(latent, noise, offsets, anchors, guidance, w_in, w_mid, w_out, t_embed, w_feat):
    features = w_feat.T
    blocks = (8, H, WIN)
    tall, square = ((HID, TAPS), BF16), ((HID, HID), BF16)
    noise_place = [
        pltpu.VMEM((C, H, WIN), F32), pltpu.SMEM((C, FEAT), F32), pltpu.SemaphoreType.DMA((2,))
    ]

    share, strength, t_embed = call(
        opening_kernel, ((GROUP, 5, H, WIN), (H, WIN), (2, HID)), "shhh",
        guidance, offsets, latent, t_embed,
        scratch=[
            pltpu.VMEM((C, H, WIN), F32), pltpu.SMEM((2,), jnp.int32),
            pltpu.SemaphoreType.DMA((3,)),
        ],
    )
    share = exchanged(share, NEAR)
    share, beside = call(
        opening_relay_kernel, ((GROUP, 13, H, WIN), (C, H, WIN)), "s", anchors, share
    )
    share = exchanged(share, FAR)

    share, own, spill, inside, outside, inverse, table, w_in_half, w_mid_half, w_mid_t, w_out_t, embed = call(
        first_kernel,
        (
            (GROUP, 9, H, WIN), blocks, blocks, blocks, blocks, (2, H, WIN), (H, WIN),
            tall, square, square, tall, (2, HID, WIN),
        ),
        "shh",
        anchors, features, noise, latent, beside, share,
        w_in.T, w_mid, w_out, t_embed,
        scratch=[pltpu.SMEM((H, WIN), F32), pltpu.SemaphoreType.DMA] + noise_place + scratches(),
        megabytes=32,
    )
    inside = swapped(inside, 0)
    outside = swapped(outside, 1)
    share = exchanged(share, NEAR)
    (share,) = call(relay_kernel, ((GROUP, 9, H, WIN),), "", share)
    share = exchanged(share, FAR)

    own, spill, squares = call(
        second_kernel, (blocks, blocks, (NDEV, 1, WIN)), "hh",
        features, noise, strength, table, share, own, spill, inside, outside,
        inverse, w_in_half, w_mid_half, w_out, w_in.T, w_mid_t, w_out_t, embed,
        scratch=noise_place + scratches(), megabytes=32,
    )
    spill_left = passed_along(spill, WA, 1)
    squares = exchanged(squares, WA)
    (out,) = call(
        closing_kernel, ((C, H, WIN),), "", strength, squares, own, spill_left, near=False
    )
    return out


def solution(mesh):
    finer = Mesh(mesh.devices.reshape(2, 4, 8, mesh.shape["ba"]), ("wa_0", "wa_1", "wa_2", "ba"))
    placed = (P("ba", None, WA), P(None, "ba", None, WA), P(WA), P(), P(), P(), P(), P(), P(), P())
    return jax.shard_map(
        local, mesh=finer, in_specs=placed, out_specs=P("ba", None, WA), check_vma=False
    )
```

```python
import math

import jax
import jax.numpy as jnp
from jax import lax
from jax.experimental import pallas as pl
from jax.experimental.pallas import tpu as pltpu
from jax.sharding import Mesh
from jax.sharding import PartitionSpec as P

C = 4
H = 8
HID = 320
FEAT = 64
WIN = 128
STRIDE = 64
NDEV = 64
NWIN = 128
TAPS = 9 * C
FIELD = H * WIN
OWN = 2
PER_TURN = 16
WA = ("wa_0", "wa_1", "wa_2")
NEAR = "wa_2"
FAR = ("wa_0", "wa_1")
GROUP = 8

TAP_SHIFTS = ((-1, -1), (-1, 0), (-1, 1), (0, -1), (0, 0), (0, 1), (1, -1), (1, 0), (1, 1))
CUMULATIVE_ALPHA = (0.35, 0.55, 0.72, 0.85, 0.93)
STABILITY = 1e-06
ELEMENTS = float(NWIN * C * H * WIN)
F32 = jnp.float32
BF16 = jnp.bfloat16


def plan(number):
    current = CUMULATIVE_ALPHA[number]
    following = CUMULATIVE_ALPHA[number + 1]
    spread = 0.3 * math.sqrt(1.0 - following)
    return (
        math.sqrt(current),
        math.sqrt(1.0 - current),
        math.sqrt(following),
        math.sqrt(1.0 - following - spread * spread),
        spread,
    )


def lanes(shape=(C, H, WIN)):
    return lax.broadcasted_iota(jnp.int32, shape, len(shape) - 1)


def shift_rows(x, by):
    if by == 0:
        return x
    row = lax.broadcasted_iota(jnp.int32, x.shape, 1)
    inside = row >= 1 if by < 0 else row < H - 1
    return jnp.where(inside, pltpu.roll(x, (-by) % H, 1), 0.0)


def shift_lanes(x, by):
    if by == 0:
        return x
    lane = lanes(x.shape)
    inside = lane >= 1 if by < 0 else lane < WIN - 1
    return jnp.where(inside, pltpu.roll(x, (-by) % WIN, 2), 0.0)


def spread_taps(x, sign, tall):
    moved = {by: shift_lanes(x, sign * by) for by in (-1, 0, 1)}
    for k, (down, right) in enumerate(TAP_SHIFTS):
        tall[32 * k : 32 * (k + 1), :] = shift_rows(moved[right], sign * down).reshape(32, WIN)
    rows = [tall[pl.ds(h, TAPS, stride=H), :] for h in range(H)]
    return jnp.concatenate(rows, axis=1).astype(BF16)


def store_taps(tall, values):
    for h in range(H):
        tall[pl.ds(h, TAPS, stride=H), :] = values[:, WIN * h : WIN * (h + 1)]


def gather_taps(tall, sign):
    total = None
    for right in (-1, 0, 1):
        part = None
        for k, (down, across) in enumerate(TAP_SHIFTS):
            if across == right:
                piece = tall[32 * k : 32 * (k + 1), :].reshape(C, H, WIN)
                piece = shift_rows(piece, sign * down)
                part = piece if part is None else part + piece
        part = shift_lanes(part, sign * right)
        total = part if total is None else total + part
    return total


def silu_and_slope(half):
    p = 1.0 + jnp.tanh(half)
    return half * p, p * (1.0 + half * (2.0 - p))


def silu(half):
    return half * (1.0 + jnp.tanh(half))


def dot(a, b):
    return lax.dot_general(a, b, (((1,), (0,)), ((), ())), preferred_element_type=F32)


def predict(windows, weights, embed, talls, slopes):
    shared = range(len(windows))
    halves = [
        (dot(weights["w_in"][...], spread_taps(windows[i], 1, talls[i])) + embed).astype(BF16)
        for i in shared
    ]

    def activated(values, kept, i):
        if i >= OWN:
            return silu(values)
        value, kept[:, i * FIELD : (i + 1) * FIELD] = silu_and_slope(values)
        return value

    middles = [
        dot(weights["w_mid"][...], activated(halves[i], slopes[0], i)).astype(BF16) for i in shared
    ]
    for i in shared:
        joined = (halves[i] + halves[i]) + activated(middles[i], slopes[1], i)
        store_taps(talls[i], dot(weights["w_out"][...], joined))
    return [gather_taps(tall, 1) for tall in talls]


def pull_back(cotangents, weights, talls, slopes):
    own = range(OWN)
    at = [slice(i * FIELD, (i + 1) * FIELD) for i in own]
    d_joined = [
        dot(weights["w_out_t"][...], spread_taps(cotangents[i], -1, talls[i])).astype(BF16)
        for i in own
    ]
    d_active = [
        dot(weights["w_mid_t"][...], d_joined[i] * slopes[1][:, at[i]]).astype(BF16) for i in own
    ]
    for i in own:
        d_hidden = d_joined[i] + d_active[i] * slopes[0][:, at[i]]
        store_taps(talls[i], dot(weights["w_in_t"][...], d_hidden))
    return [gather_taps(tall, -1) for tall in talls]


def percept_pull_back(cleans, anchor, w_feat):
    fields = [[0.5 * x[c] for c in range(C)] for x in (anchor, *cleans)]
    many = len(cleans)

    def some(turn, grads):
        grads = list(grads)
        for i in range(PER_TURN):
            f = turn * PER_TURN + i
            w = [w_feat[c, f] for c in range(C)]
            mixed = [(w[0] * x[0] + w[1] * x[1]) + (w[2] * x[2] + w[3] * x[3]) for x in fields]
            target = silu(mixed[0])
            for j in range(many):
                s, slope = silu_and_slope(mixed[1 + j])
                d = (s - target) * slope
                for c in range(C):
                    grads[j * C + c] = grads[j * C + c] + w[c] * d
        return tuple(grads)

    nothing = tuple(jnp.zeros((H, WIN), F32) for _ in range(C * many))
    grads = lax.fori_loop(0, FEAT // PER_TURN, some, nothing)
    return [jnp.stack(grads[C * j : C * (j + 1)]) * (0.5 / FEAT) for j in range(many)]


def cut(first, second, start):
    by = (WIN - start) & (WIN - 1)
    return jnp.where(
        lanes() < WIN - start, pltpu.roll(first, by, 2), pltpu.roll(second, by, 2)
    )


def place(pieces, starts):
    own, spill = 0.0, 0.0
    for piece, start in zip(pieces, starts):
        moved = pltpu.roll(piece, start, 2)
        inside = lanes() >= start
        own = own + jnp.where(inside, moved, 0.0)
        spill = spill + jnp.where(inside, 0.0, moved)
    return own, spill


def step(
    number, first, second, starts, anchor, weights, embed_ref, w_feat, scratch, prepare=lambda: None
):
    now_a, now_s, next_a, direction, _ = plan(number)
    talls, slopes = scratch[:3], scratch[3:5]
    embed = jnp.concatenate([embed_ref[number]] * (FIELD // WIN), axis=1)
    windows = [cut(first, second, start) for start in starts]
    every = windows + [anchor]
    predicted = predict(every, weights, embed, talls, slopes)
    cleans = [(w - now_s * p) * (1.0 / now_a) for w, p in zip(every, predicted)]
    prepare()
    feat_copy, feat_held = w_feat
    feat_copy.wait()
    d_cleans = percept_pull_back(cleans[:OWN], cleans[OWN], feat_held)
    pulled = pull_back([d * (-now_s / now_a) for d in d_cleans], weights, talls[:OWN], slopes)
    gradients = [d * (1.0 / now_a) + g for d, g in zip(d_cleans, pulled)]
    square = sum(jnp.sum(g * g, axis=0) for g in gradients)
    plain = [
        (next_a / now_a) * (w - now_s * p) + direction * p for w, p in zip(windows, predicted)
    ]
    plain_own, plain_spill = place(plain, starts)
    steep_own, steep_spill = place([g * (-next_a / now_a) for g in gradients], starts)
    return plain_own, plain_spill, steep_own, steep_spill, square


def scale_of(total, guidance):
    return guidance[...] * lax.rsqrt(jnp.full((H, WIN), total) * (1.0 / ELEMENTS) + STABILITY)


def opening_kernel(
    guidance, offsets, latent, t_embed, share, strength, t_embed_held, held, shifts, arrived
):
    copies = [
        pltpu.make_async_copy(latent, held, arrived.at[0]),
        pltpu.make_async_copy(offsets, shifts, arrived.at[1]),
        pltpu.make_async_copy(t_embed, t_embed_held, arrived.at[2]),
    ]
    for copy in copies:
        copy.start()
    strength[...] = jnp.full((H, WIN), guidance[0])
    for copy in copies:
        copy.wait()
    own = held[...]
    lane = lanes((H, WIN))
    known = jnp.where(
        lane == 0, shifts[0].astype(F32), jnp.where(lane == 1, shifts[1].astype(F32), 0.0)
    )
    for i in range(GROUP):
        share[i, 0:4] = own
        share[i, 4] = known


def opening_relay_kernel(anchors, got, share, beside):
    row, column = lax.axis_index(FAR), lax.axis_index(NEAR)
    owner = anchors[0] >> 1

    def block_of(device):
        return jnp.where(device >> 3 == row, got[device & 7, 0:4], 0.0)

    x, y = block_of(owner), block_of((owner + 1) & (NDEV - 1))
    right = got[(column + 1) & 7, 0:4]
    known = got[0, 4]
    for i in range(1, GROUP):
        known = known + pltpu.roll(got[i, 4], 2 * i, 1)
    known = pltpu.roll(known, 2 * GROUP * row, 1)
    beside[...] = right
    for i in range(GROUP):
        share[i, 0:4] = x
        share[i, 4:8] = y
        share[i, 8:12] = right
        share[i, 12] = known


def relay_kernel(got, share):
    total = got[0]
    for i in range(1, GROUP):
        total = total + got[i]
    for i in range(GROUP):
        share[i] = total


def turned(values, factor):
    return (values.astype(F32).T * factor).astype(BF16)


def column_of(row):
    return jnp.broadcast_to(row * 0.5, (WIN, HID)).T


def fetches(noise, w_feat, scratch):
    noise_held, feat_held, arrived = scratch[:3]
    noise_copy = pltpu.make_async_copy(noise, noise_held, arrived.at[0])
    feat_copy = pltpu.make_async_copy(w_feat, feat_held, arrived.at[1])
    noise_copy.start()
    feat_copy.start()
    return noise_copy, feat_copy, noise_held, feat_held, scratch[3:]


def offset_in(table, window):
    row = table[0:1, :]
    return jnp.sum(jnp.where(lanes((1, WIN)) == window, row, 0.0)).astype(jnp.int32)


def weights_of(refs):
    names = ("w_in", "w_mid", "w_out", "w_in_t", "w_mid_t", "w_out_t")
    return dict(zip(names, refs))


def first_kernel(
    anchors, w_feat, noise, latent, beside, shared,
    w_in_t, w_mid, w_out, t_embed,
    share, own_out, spill_out, inside, outside, inverse, table_out,
    w_in, w_mid_half, w_mid_t, w_out_t, embed, *scratch,
):
    table_held, table_arrived, *scratch = scratch
    table_copy = pltpu.make_async_copy(shared.at[:, 12, 0:1], table_held, table_arrived)
    table_copy.start()

    def summed(at):
        total = shared[0, at]
        for i in range(1, GROUP):
            total = total + shared[i, at]
        return total

    table_out[...] = summed(12)
    noise_copy, feat_copy, noise_held, feat_held, scratch = fetches(noise.at[0], w_feat, scratch)
    w_in[...] = turned(w_in_t[...], 0.5)
    w_mid_half[...] = (w_mid[...].astype(F32) * 0.5).astype(BF16)
    embed[0] = column_of(t_embed[0:1, :])

    def prepare():
        w_mid_t[...] = turned(w_mid[...], 0.25)
        w_out_t[...] = turned(w_out[...], 1.0)
        embed[1] = column_of(t_embed[1:2, :])

    weights = weights_of((w_in, w_mid_half, w_out, w_in_t, w_mid_t, w_out_t))
    me = lax.axis_index(WA)
    lane = lanes((H, WIN))
    table_copy.wait()

    def offset_of(window):
        return table_held[window >> 4, 0, window].astype(jnp.int32)

    starts = (offset_of(2 * me), STRIDE + offset_of(2 * me + 1))
    anchor_at = (anchors[0] & 1) * STRIDE + offset_of(anchors[0])
    anchor = cut(summed(pl.ds(0, 4)), summed(pl.ds(4, 4)), anchor_at)
    across = shared[((me >> 3) + 1) & 7, 8:12]
    following = jnp.where(me & 7 == 7, across, beside[...])
    plain_own, plain_spill, steep_own, steep_spill, square = step(
        0, latent[...], following, starts, anchor, weights, embed, (feat_copy, feat_held), scratch,
        prepare,
    )
    spread = plan(0)[-1]

    def covered(windows):
        count = jnp.zeros((H, WIN), F32)
        for begin in windows:
            count = count + jnp.where((lane >= begin) & (lane < begin + WIN), 1.0, 0.0)
        return 1.0 / count

    left, right = 2 * me + NWIN - 2, 2 * me + 2
    before = (
        offset_of(left & (NWIN - 1)) - WIN,
        offset_of((left + 1) & (NWIN - 1)) - STRIDE,
    )
    after = (offset_of(right & (NWIN - 1)), STRIDE + offset_of((right + 1) & (NWIN - 1)))
    inverse_own = covered(before + starts)
    inverse_next = covered((starts[0] - WIN, starts[1] - WIN) + after)
    inverse[0] = inverse_own
    inverse[1] = inverse_next
    noise_copy.wait()
    plain_own = plain_own * inverse_own + spread * noise_held[...]
    steep_own = steep_own * inverse_own
    plain_spill = plain_spill * inverse_next
    steep_spill = steep_spill * inverse_next
    own_out[0:4] = plain_own
    own_out[4:8] = steep_own
    spill_out[0:4] = plain_spill
    spill_out[4:8] = steep_spill
    odd = me & 1 == 1
    for at, own, spill in ((0, plain_own, plain_spill), (4, steep_own, steep_spill)):
        inside[at : at + 4] = jnp.where(odd, own, spill)
        outside[at : at + 4] = jnp.where(odd, spill, own)

    owner = anchors[1] >> 1
    next_at = (anchors[1] & 1) * STRIDE + offset_of(anchors[1])
    here, ahead, behind = (
        me == owner, me == (owner + 1) & (NDEV - 1), me == (owner - 1) & (NDEV - 1)
    )

    def portion(own, spill):
        x = jnp.where(here, own, jnp.where(behind, spill, 0.0))
        y = jnp.where(here, spill, jnp.where(ahead, own, 0.0))
        return cut(x, y, next_at)

    plain_part = portion(plain_own, plain_spill)
    steep_part = portion(steep_own, steep_spill)
    for i in range(GROUP):
        share[i, 0:4] = plain_part
        share[i, 4:8] = steep_part
        share[i, 8] = square


def second_kernel(
    w_feat, noise, guidance, table, shared, own_in, spill_in, inside, outside, inverse,
    w_in, w_mid, w_out, w_in_t, w_mid_t, w_out_t, embed,
    own_out, spill_out, square_out, *scratch,
):
    noise_copy, feat_copy, noise_held, feat_held, scratch = fetches(noise.at[1], w_feat, scratch)
    me = lax.axis_index(WA)
    starts = (offset_in(table, 2 * me), STRIDE + offset_in(table, 2 * me + 1))
    weights = weights_of((w_in, w_mid, w_out, w_in_t, w_mid_t, w_out_t))
    total = shared[0]
    for i in range(1, GROUP):
        total = total + shared[i]
    scale = scale_of(jnp.sum(total[8]), guidance)
    spread = plan(1)[-1]
    anchor = total[0:4] + scale * total[4:8]
    odd = me & 1 == 1
    own = own_in[...] + jnp.where(odd, inside[...], outside[...])
    beyond = spill_in[...] + jnp.where(odd, outside[...], inside[...])
    first = own[0:4] + scale * own[4:8]
    second = beyond[0:4] + scale * beyond[4:8]
    plain_own, plain_spill, steep_own, steep_spill, square = step(
        1, first, second, starts, anchor, weights, embed, (feat_copy, feat_held), scratch
    )
    noise_copy.wait()
    own_out[0:4] = plain_own * inverse[0] + spread * noise_held[...]
    own_out[4:8] = steep_own * inverse[0]
    spill_out[0:4] = plain_spill * inverse[1]
    spill_out[4:8] = steep_spill * inverse[1]
    row = jnp.sum(square, axis=0, keepdims=True)
    square_out[...] = jnp.broadcast_to(row[None], (NDEV, 1, WIN))


def closing_kernel(guidance, squares, own_in, spill_left, out):
    scale = scale_of(jnp.sum(squares[...]), guidance)
    own = own_in[...] + spill_left[...]
    out[...] = own[0:4] + scale * own[4:8]


def call(kernel, shapes, spaces, *args, scratch=(), megabytes=4, near=True):
    kinds = {"s": pltpu.SMEM, "h": pltpu.HBM, "v": pltpu.VMEM}
    in_specs = [
        pl.BlockSpec(memory_space=kinds[letter]) for letter in spaces.ljust(len(args), "v")
    ]
    args = [
        pltpu.with_memory_space_constraint(arg, pltpu.HBM) if letter == "h" else arg
        for arg, letter in zip(args, spaces.ljust(len(args), "v"))
    ]
    return pl.pallas_call(
        kernel,
        out_shape=[
            (pltpu.VMEM if near else jax.ShapeDtypeStruct)(
                *(shape if isinstance(shape[0], tuple) else (shape, F32))
            )
            for shape in shapes
        ],
        in_specs=in_specs,
        out_specs=[pl.BlockSpec(memory_space=pltpu.VMEM) for _ in shapes],
        scratch_shapes=scratch,
        compiler_params=pltpu.CompilerParams(vmem_limit_bytes=megabytes << 20),
    )(*args)


def scratches():
    return (
        [pltpu.VMEM((8 * TAPS, WIN), F32)] * (OWN + 1)
        + [pltpu.VMEM((HID, OWN * FIELD), BF16)] * 2
    )


def exchanged(shares, axes):
    return lax.all_to_all(shares, axes, split_axis=0, concat_axis=0, tiled=True)


def passed_along(shard, axes, by):
    length = lax.axis_size(axes)
    return lax.ppermute(shard, axes, [(i, (i + by) % length) for i in range(length)])


def swapped(shard, first):
    pairs = [((first + i) % NDEV, (first + (i ^ 1)) % NDEV) for i in range(NDEV)]
    return lax.ppermute(shard, WA, pairs)


def local(latent, noise, offsets, anchors, guidance, w_in, w_mid, w_out, t_embed, w_feat):
    features = w_feat.T
    blocks = (8, H, WIN)
    tall, square = ((HID, TAPS), BF16), ((HID, HID), BF16)
    noise_place = [
        pltpu.VMEM((C, H, WIN), F32), pltpu.SMEM((C, FEAT), F32), pltpu.SemaphoreType.DMA((2,))
    ]

    share, strength, t_embed = call(
        opening_kernel, ((GROUP, 5, H, WIN), (H, WIN), (2, HID)), "shhh",
        guidance, offsets, latent, t_embed,
        scratch=[
            pltpu.VMEM((C, H, WIN), F32), pltpu.SMEM((2,), jnp.int32),
            pltpu.SemaphoreType.DMA((3,)),
        ],
    )
    share = exchanged(share, NEAR)
    share, beside = call(
        opening_relay_kernel, ((GROUP, 13, H, WIN), (C, H, WIN)), "s", anchors, share
    )
    share = exchanged(share, FAR)

    share, own, spill, inside, outside, inverse, table, w_in_half, w_mid_half, w_mid_t, w_out_t, embed = call(
        first_kernel,
        (
            (GROUP, 9, H, WIN), blocks, blocks, blocks, blocks, (2, H, WIN), (H, WIN),
            tall, square, square, tall, (2, HID, WIN),
        ),
        "shh",
        anchors, features, noise, latent, beside, share,
        w_in.T, w_mid, w_out, t_embed,
        scratch=[pltpu.SMEM((GROUP, 1, WIN), F32), pltpu.SemaphoreType.DMA]
        + noise_place
        + scratches(),
        megabytes=32,
    )
    outside = swapped(outside, 1)
    inside = swapped(inside, 0)
    share = exchanged(share, NEAR)
    (share,) = call(relay_kernel, ((GROUP, 9, H, WIN),), "", share)
    share = exchanged(share, FAR)

    own, spill, squares = call(
        second_kernel, (blocks, blocks, (NDEV, 1, WIN)), "hh",
        features, noise, strength, table, share, own, spill, inside, outside,
        inverse, w_in_half, w_mid_half, w_out, w_in.T, w_mid_t, w_out_t, embed,
        scratch=noise_place + scratches(), megabytes=32,
    )
    spill_left = passed_along(spill, WA, 1)
    squares = exchanged(squares, WA)
    (out,) = call(
        closing_kernel, ((C, H, WIN),), "", strength, squares, own, spill_left, near=False
    )
    return out


def solution(mesh):
    finer = Mesh(mesh.devices.reshape(2, 4, 8, mesh.shape["ba"]), ("wa_0", "wa_1", "wa_2", "ba"))
    placed = (P("ba", None, WA), P(None, "ba", None, WA), P(WA), P(), P(), P(), P(), P(), P(), P())
    return jax.shard_map(
        local, mesh=finer, in_specs=placed, out_specs=P("ba", None, WA), check_vma=False
    )
```
